256 devices in a mesh: lat: 128 (over x, z, y), lev: 2 (over core).
Axes of the slice: x: 4, y: 4, z: 8, core: 2. Of those that a mesh axis runs over, the one named last changes fastest.
Arguments:
- fields: float32 [1280, 3, 16, 2560], P('lat', None, 'lev'), may hold values from 0.1 to 5
- lat_fraction: float32 [1280], P('lat'), may hold values from 0 to 1
- lon_fraction: float32 [1280], P('lat'), may hold values from 0 to 1
- lon_shift: int32 [1280], P('lat'), may hold values from 0 to 2559
- departure_row: int32 [1280], P('lat'), may hold values from 1 to 1277, as said below
- extents: int32 [128, 2], P('lat'), may hold values from 1 to 4
Outputs:
- advected: float32 [1280, 3, 16, 2560], P('lat', None, 'lev')
The draws below stay inside these ranges and needn't reach their ends.
Inputs may be any that keep to these rules, and one draw needn't show every extreme that they name: departure_row[r] lies within 39 rows of r.
All inputs are finite; a program needn't handle non-finite values.
Results may differ from the reference program's by a relative error of at most 0.0003.
Values sent between devices are 32-bit elements; how exact they have to be, the bound alone decides.
No kernel may reach another device: no remote copies, remote signals or barrier semaphores. Data moves between devices by JAX's collectives and lax.ppermute only.
A program may use at most 128 MiB of HBM per device.

```python
import math
import jax
import jax.numpy as jnp
from jax import lax

ROWS = 10
LON = 2560
FIELDS = 3
REACH = 4
NLAT = 1280
LEV = 16
BANDS = 128


def band_phase(key):
    return jax.random.randint(jax.random.fold_in(key, 911), (), 0, 8 * ROWS)


def draw_fields(key, part):
    row_phase = band_phase(key)
    shifted_rows = (jnp.arange(NLAT, dtype=jnp.int32) + row_phase) % (8 * ROWS)
    row_angle = 2.0 * math.pi * shifted_rows.astype(jnp.float32) / (8 * ROWS)
    full_shape = (NLAT, FIELDS, LEV, LON)
    gain_row = jnp.exp(-0.5 * jnp.sin(row_angle))
    rough_part = jax.random.uniform(jax.random.fold_in(key, 23), full_shape, jnp.float32, 0.5, 2.0)
    return (gain_row[:, None, None, None] * rough_part).astype(jnp.float32)


def draw_departure_row(key, part):
    row_phase = band_phase(key)
    row_ids = jnp.arange(NLAT, dtype=jnp.int32)
    shifted_rows = (row_ids + row_phase) % (8 * ROWS)
    row_drift = jnp.clip(2 * (2 * ROWS - jnp.abs(shifted_rows - 4 * ROWS)), -2 * ROWS, 2 * ROWS)
    row_noise = jax.random.randint(jax.random.fold_in(key, 17), (NLAT,), -2 * ROWS, 2 * ROWS + 1)
    offsets = jnp.clip(row_drift + row_noise, -REACH * ROWS + 1, REACH * ROWS - 2)
    spread = jax.random.randint(jax.random.fold_in(key, 29), (NLAT,), 0, 1 << 20)
    north_offset = -(1 + spread % (REACH * ROWS - 1))
    south_offset = 1 + spread % (REACH * ROWS - 2)
    position = row_ids % ROWS
    offsets = jnp.where(position == 0, north_offset, offsets)
    offsets = jnp.where(position == ROWS - 1, south_offset, offsets)
    return jnp.clip(row_ids + offsets, 1, NLAT - 3).astype(jnp.int32)


def plant(array, rng, low, largest):
    spot = [jax.random.randint(jax.random.fold_in(rng, axis), (), 0, length) for axis, length in enumerate(array.shape)]
    widest = array.shape.index(max(array.shape))
    next_to = spot[:widest] + [(spot[widest] + 1) % array.shape[widest]] + spot[widest + 1:]
    return array.at[tuple(spot)].set(low).at[tuple(next_to)].set(largest)


def level_of(stream_key, shape, pieces, smallest, high):
    def one(axis_at, blocks):
        heights = jax.random.uniform(jax.random.fold_in(jax.random.fold_in(stream_key, 6), axis_at), (blocks,), jnp.float32, smallest / len(pieces), high / len(pieces))
        return jnp.repeat(jnp.exp(heights), shape[axis_at] // blocks).reshape((-1,) + (1,) * (len(shape) - axis_at - 1))

    gain = one(*pieces[0])
    for cut in pieces[1:]:
        gain = gain * one(*cut)
    return gain


def setup_inputs(seed: int = 0) -> dict:
    key_of = jax.random.split(jax.random.key(seed), 7)
    return {
        "fields": draw_fields(jax.random.fold_in(key_of[6], 71), 0),
        "lat_fraction": jnp.clip(1.0 * jax.random.uniform(key_of[1], (NLAT,), jnp.float32) ** level_of(key_of[1], (NLAT,), ((0, 128),), -0.2, 0.2), 0.0, 1.0),
        "lon_fraction": jnp.clip(1.0 * jax.random.uniform(key_of[2], (NLAT,), jnp.float32) ** level_of(key_of[2], (NLAT,), ((0, 128),), -0.2, 0.2), 0.0, 1.0),
        "lon_shift": plant(jax.random.randint(key_of[3], (NLAT,), 0, LON), jax.random.fold_in(key_of[3], 1), 0, LON - 1).astype(jnp.int32),
        "departure_row": draw_departure_row(jax.random.fold_in(key_of[6], 71), 0),
        "extents": plant(jax.random.randint(key_of[5], (BANDS, 2), 1, REACH + 1), jax.random.fold_in(key_of[5], 1), 1, REACH).astype(jnp.int32),
    }


def cubic_weights(fraction):
    return jnp.stack([-fraction * (fraction - 1.0) * (fraction - 2.0) / 6.0,
                      (fraction + 1.0) * (fraction - 1.0) * (fraction - 2.0) / 2.0,
                      -(fraction + 1.0) * fraction * (fraction - 2.0) / 2.0,
                      (fraction + 1.0) * fraction * (fraction - 1.0) / 6.0])


def along_lon(column, lon_w, shift_value):
    lon_count = column.shape[-1]
    doubled = jnp.concatenate([column, column], axis=-1)
    result = jnp.zeros_like(column)
    for offset in range(4):
        first = ((shift_value + offset - 1) % lon_count).astype(jnp.int32)
        result = result + lon_w[offset] * lax.dynamic_slice_in_dim(doubled, first, lon_count, 2)
    return result


def reference(fields, lat_fraction, lon_fraction, lon_shift, departure_row, extents):
    row_ids = jnp.arange(NLAT, dtype=jnp.int32)
    band_ids = row_ids // ROWS
    low_bound = band_ids * ROWS - extents[band_ids, 0] * ROWS + 1
    high_bound = band_ids * ROWS + ROWS - 3 + extents[band_ids, 1] * ROWS
    departure = jnp.clip(jnp.clip(departure_row, low_bound, high_bound), 1, NLAT - 3).astype(jnp.int32)

    def one_row(inputs):
        dep_value, lat_t, lon_t, shift_value = inputs
        row_block = lax.dynamic_slice_in_dim(fields, (dep_value - 1).astype(jnp.int32), 4, 0)
        lat_w = cubic_weights(lat_t)
        column = lat_w[0] * row_block[0] + lat_w[1] * row_block[1] + lat_w[2] * row_block[2] + lat_w[3] * row_block[3]
        return along_lon(column, cubic_weights(lon_t), shift_value)

    moved = lax.map(one_row, (departure, lat_fraction, lon_fraction, lon_shift))
    area = jnp.cos(math.pi * (row_ids.astype(jnp.float32) + 0.5) / NLAT - math.pi / 2.0)
    mass_before = jnp.sum(area[:, None, None, None] * fields, axis=(0, 2, 3))
    mass_after = jnp.sum(area[:, None, None, None] * moved, axis=(0, 2, 3))
    return moved * (mass_before / mass_after)[None, :, None, None]
```

```python
import math
from functools import partial

import jax
import jax.numpy as jnp
from jax import lax
from jax.experimental import pallas as pl
from jax.experimental.pallas import tpu as pltpu
from jax.sharding import Mesh
from jax.sharding import PartitionSpec as P

LAT = ("lat_0", "lat_1", "lat_2")
ROWS = 10
RING = 4
GROUP = RING * ROWS
FIELDS = 3
LANES = 128
QUARTER = 5
TILES = RING * QUARTER
LON = TILES * LANES
UNITS = FIELDS * QUARTER
CUTS = (0, 4, 9, 13, 15)
CHUNKS = tuple(zip(CUTS[:-1], CUTS[1:]))
EXTRA = 1
VMEM_LIMIT = 48 * 1024 * 1024


def cubic_weights(fraction):
    return (
        -fraction * (fraction - 1.0) * (fraction - 2.0) / 6.0,
        (fraction + 1.0) * (fraction - 1.0) * (fraction - 2.0) / 2.0,
        -(fraction + 1.0) * fraction * (fraction - 2.0) / 2.0,
        (fraction + 1.0) * fraction * (fraction - 1.0) / 6.0,
    )


def extra_tiles(chunk):
    return EXTRA if chunk == 0 else 0


def pack_kernel(fields_ref, info_ref, *piece_refs):
    sub = lax.broadcasted_iota(jnp.int32, (ROWS, LANES), 0)
    lane = lax.broadcasted_iota(jnp.int32, (ROWS, LANES), 1)
    info = info_ref[...]
    info_sub = lax.broadcasted_iota(jnp.int32, (8, LANES), 0)
    for field in range(FIELDS):
        total = fields_ref[:, field, :, 0:LANES]
        for tile in range(1, TILES):
            total = total + fields_ref[:, field, :, tile * LANES : (tile + 1) * LANES]
        by_row = jnp.sum(jnp.sum(total, axis=1), axis=1, keepdims=True)
        in_lanes = jnp.sum(jnp.where(sub == lane, by_row, 0.0), axis=0, keepdims=True)
        info = jnp.where(info_sub == 3 + field, in_lanes, info)
    for chunk, (first, last) in enumerate(CHUNKS):
        width = last - first
        for owner in range(RING):
            for row in range(ROWS):
                for unit in range(first, last):
                    field, tile = divmod(unit, QUARTER)
                    start = (owner * QUARTER + tile) * LANES
                    piece_refs[chunk][owner, row * width + unit - first] = fields_ref[
                        row, field, :, start : start + LANES
                    ]
            if extra_tiles(chunk):
                piece_refs[chunk][owner, ROWS * width] = info


def column_kernel(width, start_ref, weight_ref, north_ref, own_ref, south_ref, out_ref, rows_ref):
    count = width * ROWS
    for place, ref in enumerate((north_ref, own_ref, south_ref)):
        for band in range(RING):
            rows_ref[pl.ds((place * RING + band) * count, count)] = ref[band, :count]

    def one_row(row, carry):
        for band in range(RING):
            first = start_ref[band, row]
            total = weight_ref[0, band, row] * rows_ref[pl.ds(first * width, width)]
            for step in range(1, 4):
                total = total + weight_ref[step, band, row] * rows_ref[pl.ds((first + step) * width, width)]
            out_ref[band, pl.ds(row * width, width)] = total
        return carry

    lax.fori_loop(0, ROWS, one_row, 0)


def finish_kernel(shift_ref, weight_ref, ratio_ref, *refs):
    piece_refs, out_ref, turned_ref = refs[: len(CHUNKS)], refs[-2], refs[-1]
    lane = lax.broadcasted_iota(jnp.int32, (8, LANES), 1)
    where_unit = {}
    for chunk, (first, last) in enumerate(CHUNKS):
        for unit in range(first, last):
            where_unit[unit] = (chunk, unit - first, last - first)

    def one_row(row, carry):
        base = shift_ref[row]
        base = jnp.where(base == 0, LON - 1, base - 1)
        whole = base // LANES
        part = base - whole * LANES
        back = LANES - part
        for field in range(FIELDS):
            for owner in range(RING):
                for tile in range(QUARTER):
                    chunk, at, width = where_unit[field * QUARTER + tile]
                    piece = piece_refs[chunk][owner, row * width + at]
                    turned_ref[owner * QUARTER + tile] = piece
                    turned_ref[TILES + owner * QUARTER + tile] = piece
            scale = ratio_ref[field]
            weights = [weight_ref[step, row] * scale for step in range(4)]
            rolled = [pltpu.roll(turned_ref[whole + tile], back, 1) for tile in range(TILES)]
            rolled.append(rolled[0])
            lined = [jnp.where(lane < back, rolled[tile], rolled[tile + 1]) for tile in range(TILES)]
            lined.append(lined[0])
            total = [weights[0] * lined[tile] for tile in range(TILES)]
            for step in range(1, 4):
                moved = [pltpu.roll(lined[tile], LANES - step, 1) for tile in range(TILES)]
                moved.append(moved[0])
                for tile in range(TILES):
                    near = jnp.where(lane < LANES - step, moved[tile], moved[tile + 1])
                    total[tile] = total[tile] + weights[step] * near
            for tile in range(TILES):
                out_ref[row, field, :, tile * LANES : (tile + 1) * LANES] = total[tile]
        return carry

    lax.fori_loop(0, ROWS, one_row, 0)


def turn(array, axis, distance):
    count = lax.axis_size(axis)
    return lax.ppermute(array, axis, [(i, (i + distance) % count) for i in range(count)])


def total_over(array, axis):
    pieces = [turn(array, axis, distance) for distance in range(1, lax.axis_size(axis))]
    for piece in pieces:
        array = array + piece
    return array


def per_device(fields, lat_fraction, lon_fraction, lon_shift, departure_row, extents):
    vmem = pl.BlockSpec(memory_space=pltpu.VMEM)
    smem = pl.BlockSpec(memory_space=pltpu.SMEM)
    params = pltpu.CompilerParams(vmem_limit_bytes=VMEM_LIMIT)
    band_index = lax.axis_index(LAT)
    group_index = lax.axis_index(LAT[:2])
    total_rows = lax.axis_size(LAT) * ROWS
    first_row = band_index * ROWS
    group_row = group_index * GROUP
    low_bound = first_row - extents[0, 0] * ROWS + 1
    high_bound = first_row + ROWS - 3 + extents[0, 1] * ROWS
    departure = jnp.clip(jnp.clip(departure_row, low_bound, high_bound), 1, total_rows - 3)
    start = departure - 1 - (group_row - GROUP)
    lon_w = jnp.stack(cubic_weights(lon_fraction))
    info = jnp.zeros((8, LANES), jnp.float32)
    info = info.at[0, :ROWS].set(start.astype(jnp.float32))
    info = info.at[1, :ROWS].set(lat_fraction)
    info = info.at[2, :ROWS].set(lon_w[0] + lon_w[1] + lon_w[2] + lon_w[3])

    pieces = pl.pallas_call(
        pack_kernel,
        out_shape=[
            jax.ShapeDtypeStruct((RING, ROWS * (last - first) + extra_tiles(chunk), 8, LANES), jnp.float32)
            for chunk, (first, last) in enumerate(CHUNKS)
        ],
        in_specs=[vmem, vmem],
        out_specs=[vmem] * len(CHUNKS),
        compiler_params=params,
        name="pack",
    )(fields, info)

    own = [lax.all_to_all(piece, LAT[2], 0, 0) for piece in pieces]
    north = [turn(piece, LAT[:2], 1) for piece in own]
    south = [turn(piece, LAT[:2], -1) for piece in own]

    ring_info = own[0][:, -1, :, :ROWS]
    ring_start = ring_info[:, 0].astype(jnp.int32)
    ring_weight = jnp.stack(cubic_weights(ring_info[:, 1]))

    gathered = []
    for chunk, (first, last) in enumerate(CHUNKS):
        width = last - first
        columns = pl.pallas_call(
            partial(column_kernel, width),
            out_shape=jax.ShapeDtypeStruct((RING, ROWS * width, 8, LANES), jnp.float32),
            in_specs=[smem, smem, vmem, vmem, vmem],
            out_specs=vmem,
            scratch_shapes=[pltpu.VMEM((3 * GROUP * width, 8, LANES), jnp.float32)],
            compiler_params=params,
            name="column",
        )(ring_start, ring_weight, north[chunk], own[chunk], south[chunk])
        gathered.append(lax.all_to_all(columns, LAT[2], 0, 0))

    ring_rows = group_row + jnp.arange(GROUP, dtype=jnp.int32).reshape(RING, ROWS)
    area = jnp.cos(math.pi * (ring_rows.astype(jnp.float32) + 0.5) / total_rows - math.pi / 2.0)
    sums = jnp.stack([part[0][:, -1, 3 : 3 + FIELDS, :ROWS] for part in (north, own, south)])
    spots = jnp.arange(3 * GROUP, dtype=jnp.int32).reshape(3, RING, ROWS)
    factor = jnp.zeros((3, RING, ROWS), jnp.float32)
    for step in range(4):
        hit = (ring_start + step)[None, None, None] == spots[..., None, None]
        share = area * ring_info[:, 2] * ring_weight[step]
        factor = factor + jnp.sum(jnp.where(hit, share[None, None, None], 0.0), axis=(3, 4))
    after = jnp.sum(factor[:, :, None, :] * sums, axis=(0, 1, 3))
    before = jnp.sum(area[:, None, :] * sums[1], axis=(0, 2))
    mass = jnp.concatenate([before, after])
    mass = total_over(mass, "lev")
    mass = total_over(mass, LAT[0])
    mass = total_over(mass, LAT[1])
    ratio = mass[:FIELDS] / mass[FIELDS:]

    return pl.pallas_call(
        finish_kernel,
        out_shape=jax.ShapeDtypeStruct(fields.shape, jnp.float32),
        in_specs=[smem, smem, smem] + [vmem] * len(CHUNKS),
        out_specs=vmem,
        scratch_shapes=[pltpu.VMEM((2 * TILES, 8, LANES), jnp.float32)],
        compiler_params=params,
        name="finish",
    )(lon_shift, lon_w, ratio, *gathered)


def solution(mesh):
    finer = Mesh(mesh.devices.reshape(4, 8, 4, mesh.shape["lev"]), LAT + ("lev",))
    placed = (P(LAT, None, "lev", None), P(LAT), P(LAT), P(LAT), P(LAT), P(LAT, None))
    return jax.shard_map(
        per_device,
        mesh=finer,
        in_specs=placed,
        out_specs=P(LAT, None, "lev", None),
        check_vma=False,
    )
```

```python
import math
from functools import partial

import jax
import jax.numpy as jnp
from jax import lax
from jax.experimental import pallas as pl
from jax.experimental.pallas import tpu as pltpu
from jax.sharding import Mesh
from jax.sharding import PartitionSpec as P


LAT = ("lat_0", "lat_1", "lat_2")
ROWS = 10
RING = 4
GROUP = RING * ROWS
FIELDS = 3
LANES = 128
QUARTER = 5
TILES = RING * QUARTER
LON = TILES * LANES
CUTS = (0, 2, 6, 12, 15)
CHUNKS = tuple(zip(CUTS[:-1], CUTS[1:]))
INFO_CHUNK = 1
VMEM_LIMIT = 14 * 1024 * 1024


VMEM = pl.BlockSpec(memory_space=pltpu.VMEM)
SMEM = pl.BlockSpec(memory_space=pltpu.SMEM)
ANY = pl.BlockSpec(memory_space=pl.ANY)


def cubic_weights(fraction):
    return (
        -fraction * (fraction - 1.0) * (fraction - 2.0) / 6.0,
        (fraction + 1.0) * (fraction - 1.0) * (fraction - 2.0) / 2.0,
        -(fraction + 1.0) * fraction * (fraction - 2.0) / 2.0,
        (fraction + 1.0) * fraction * (fraction - 1.0) / 6.0,
    )


def around(place, distance):
    return lax.rem(place + RING + distance, RING)


def tile_count(chunk):
    first, last = CHUNKS[chunk]
    return ROWS * (last - first) + (1 if chunk == INFO_CHUNK else 0)


def copy_units(fields_ref, field_base, chunk, piece_refs):
    first, last = CHUNKS[chunk]
    width = last - first
    place = lax.axis_index(LAT[2])
    for distance in range(RING):
        owner = around(place, distance)
        for unit in range(first, last):
            field, tile = divmod(unit, QUARTER)
            start = pl.multiple_of((owner * QUARTER + tile) * LANES, LANES)
            for row in range(ROWS):
                piece_refs[distance][row * width + unit - first] = fields_ref[
                    row, field - field_base, :, pl.ds(start, LANES)
                ]


def pack_first(fields_ref, *piece_refs):
    copy_units(fields_ref, 0, 0, piece_refs)


def pack_rest(departure_ref, extents_ref, lat_ref, lon_ref, fields_ref, *piece_refs):
    band = lax.axis_index(LAT)
    first_row = band * ROWS
    group_row = lax.axis_index(LAT[:2]) * GROUP
    low_bound = first_row - extents_ref[0, 0] * ROWS + 1
    high_bound = first_row + ROWS - 3 + extents_ref[0, 1] * ROWS
    info_sub = lax.broadcasted_iota(jnp.int32, (8, LANES), 0)
    info_lane = lax.broadcasted_iota(jnp.int32, (8, LANES), 1)
    starts = jnp.zeros((8, LANES), jnp.int32)
    info = jnp.zeros((8, LANES), jnp.float32)
    for row in range(ROWS):
        departure = jnp.clip(departure_ref[row], low_bound, high_bound)
        departure = jnp.clip(departure, 1, RING * 32 * ROWS - 3)
        here = info_lane == row
        starts = jnp.where(here, departure - 1 - (group_row - GROUP), starts)
        info = jnp.where(here & (info_sub == 1), lat_ref[row], info)
        info = jnp.where(here & (info_sub == 2), lon_ref[row], info)
    info = jnp.where(info_sub == 0, starts.astype(jnp.float32), info)
    sub = lax.broadcasted_iota(jnp.int32, (ROWS, LANES), 0)
    lane = lax.broadcasted_iota(jnp.int32, (ROWS, LANES), 1)
    for field in range(FIELDS):
        total = fields_ref[:, field, :, 0:LANES]
        for tile in range(1, TILES):
            total = total + fields_ref[:, field, :, tile * LANES : (tile + 1) * LANES]
        by_row = jnp.sum(jnp.sum(total, axis=1), axis=1, keepdims=True)
        in_lanes = jnp.sum(jnp.where(sub == lane, by_row, 0.0), axis=0, keepdims=True)
        info = jnp.where(info_sub == 3 + field, in_lanes, info)
    for chunk in range(1, len(CHUNKS)):
        refs = piece_refs[(chunk - 1) * RING : chunk * RING]
        copy_units(fields_ref, 0, chunk, refs)
        if chunk == INFO_CHUNK:
            for ref in refs:
                ref[tile_count(chunk) - 1] = info


def join_kernel(*refs):
    for distance in range(RING):
        refs[RING][distance] = refs[distance][...]


def column_kernel(width, start_ref, weight_ref, north_ref, own_ref, south_ref, *refs):
    out_refs, rows_ref = refs[:RING], refs[RING]
    count = width * ROWS
    place = lax.axis_index(LAT[2])
    for distance in range(RING):
        band = around(place, -distance)
        for side, ref in enumerate((north_ref, own_ref, south_ref)):
            rows_ref[pl.ds((side * RING + band) * count, count)] = ref[distance, :count]

    def one_row(row, carry):
        for distance in range(RING):
            source = (RING - distance) % RING
            first = start_ref[source, row]
            total = weight_ref[0, source, row] * rows_ref[pl.ds(first * width, width)]
            for step in range(1, 4):
                total = total + weight_ref[step, source, row] * rows_ref[pl.ds((first + step) * width, width)]
            out_refs[distance][pl.ds(row * width, width)] = total
        return carry

    lax.fori_loop(0, ROWS, one_row, 0)


def field_units(field):
    found = []
    for tile in range(QUARTER):
        unit = field * QUARTER + tile
        for chunk, (first, last) in enumerate(CHUNKS):
            if first <= unit < last:
                found.append((chunk, unit - first, last - first))
    return found


def field_chunks(field):
    return sorted({chunk for chunk, _, _ in field_units(field)})


def finish_kernel(field, rows, shift_ref, weight_ref, ratio_ref, *refs):
    out_ref, turned_ref = refs[-2], refs[-1]
    chunks = field_chunks(field)
    place = lax.axis_index(LAT[2])
    owners = [around(place, -distance) for distance in range(RING)]
    lane = lax.broadcasted_iota(jnp.int32, (8, LANES), 1)
    row_base = pl.program_id(0) * rows
    scale = ratio_ref[field]

    def one_row(step_row, carry):
        row = row_base + step_row
        base = shift_ref[row]
        base = jnp.where(base == 0, LON - 1, base - 1)
        whole = base // LANES
        back = LANES - (base - whole * LANES)
        for distance in range(RING):
            for tile, (chunk, at, width) in enumerate(field_units(field)):
                piece = refs[chunks.index(chunk) * RING + distance][row * width + at]
                turned_ref[owners[distance] * QUARTER + tile] = piece
                turned_ref[TILES + owners[distance] * QUARTER + tile] = piece
        weights = [weight_ref[step, row] * scale for step in range(4)]
        rolled = [pltpu.roll(turned_ref[whole + tile], back, 1) for tile in range(TILES)]
        rolled.append(rolled[0])
        lined = [jnp.where(lane < back, rolled[tile], rolled[tile + 1]) for tile in range(TILES)]
        lined.append(lined[0])
        total = [weights[0] * lined[tile] for tile in range(TILES)]
        for step in range(1, 4):
            moved = [pltpu.roll(lined[tile], LANES - step, 1) for tile in range(TILES)]
            moved.append(moved[0])
            for tile in range(TILES):
                near = jnp.where(lane < LANES - step, moved[tile], moved[tile + 1])
                total[tile] = total[tile] + weights[step] * near
        for tile in range(TILES):
            out_ref[step_row, 0, :, tile * LANES : (tile + 1) * LANES] = total[tile]
        return carry

    lax.fori_loop(0, rows, one_row, 0)


def turn(array, axis, distance):
    count = lax.axis_size(axis)
    return lax.ppermute(array, axis, [(i, (i + distance) % count) for i in range(count)])


def exchange(pieces):
    return [pieces[0]] + [turn(pieces[distance], LAT[2], distance) for distance in range(1, RING)]


def tiles(*shape):
    return jax.ShapeDtypeStruct((*shape, 8, LANES), jnp.float32)


def per_device(fields, lat_fraction, lon_fraction, lon_shift, departure_row, extents):
    params = pltpu.CompilerParams(vmem_limit_bytes=VMEM_LIMIT)
    last_chunk = len(CHUNKS)

    width = CHUNKS[0][1]
    first_pieces = pl.pallas_call(
        pack_first,
        grid=(1,),
        out_shape=[tiles(ROWS * width)] * RING,
        in_specs=[pl.BlockSpec((ROWS, 1, 8, LON), lambda i: (0, 0, 0, 0))],
        out_specs=[pl.BlockSpec((ROWS * width, 8, LANES), lambda i: (0, 0, 0))] * RING,
        compiler_params=params,
        name="pack_a",
    )(fields)
    rest = pl.pallas_call(
        pack_rest,
        out_shape=[tiles(tile_count(chunk)) for chunk in range(1, last_chunk) for _ in range(RING)],
        in_specs=[SMEM] * 4 + [VMEM],
        out_specs=[VMEM] * (RING * (last_chunk - 1)),
        compiler_params=params,
        name="pack_b",
    )(departure_row, extents, lat_fraction, lon_fraction, fields)
    pieces = [first_pieces] + [rest[i * RING : (i + 1) * RING] for i in range(last_chunk - 1)]

    own, north, south = [], [], []
    for chunk in range(last_chunk):
        received = exchange(pieces[chunk])
        joined = pl.pallas_call(
            join_kernel,
            out_shape=tiles(RING, tile_count(chunk)),
            in_specs=[VMEM] * RING,
            out_specs=VMEM,
            compiler_params=params,
            name="join",
        )(*received)
        north.append(turn(joined, LAT[:2], 1))
        south.append(turn(joined, LAT[:2], -1))
        own.append(joined)

    ring_info = own[INFO_CHUNK][:, -1, :, :ROWS]
    ring_start = ring_info[:, 0].astype(jnp.int32)
    ring_weight = jnp.stack(cubic_weights(ring_info[:, 1]))

    gathered = []
    for chunk, (first, last) in enumerate(CHUNKS):
        width = last - first
        columns = pl.pallas_call(
            partial(column_kernel, width),
            out_shape=[tiles(ROWS * width)] * RING,
            in_specs=[SMEM, SMEM, VMEM, VMEM, VMEM],
            out_specs=[VMEM] * RING,
            scratch_shapes=[pltpu.VMEM((3 * GROUP * width, 8, LANES), jnp.float32)],
            compiler_params=params,
            name="column",
        )(ring_start, ring_weight, north[chunk], own[chunk], south[chunk])
        gathered.append(exchange(columns))

    total_rows = lax.axis_size(LAT) * ROWS
    group_row = lax.axis_index(LAT[:2]) * GROUP
    bands = around(lax.axis_index(LAT[2]), -jnp.arange(RING, dtype=jnp.int32))
    ring_rows = bands[:, None] * ROWS + jnp.arange(ROWS, dtype=jnp.int32)[None]
    area = jnp.cos(math.pi * ((group_row + ring_rows).astype(jnp.float32) + 0.5) / total_rows - math.pi / 2.0)
    sums = [part[INFO_CHUNK][:, -1, 3 : 3 + FIELDS, :ROWS] for part in (north, own, south)]
    lon_total = sum(cubic_weights(ring_info[:, 2]))
    before = jnp.sum(area[:, None, :] * sums[1], axis=(0, 2))
    after = jnp.zeros((FIELDS,), jnp.float32)
    for side in range(3):
        spots = side * GROUP + ring_rows
        factor = jnp.zeros((RING, ROWS), jnp.float32)
        for step in range(4):
            hit = (ring_start + step)[None, None] == spots[..., None, None]
            share = area * lon_total * ring_weight[step]
            factor = factor + jnp.sum(jnp.where(hit, share[None, None], 0.0), axis=(2, 3))
        after = after + jnp.sum(factor[:, None, :] * sums[side], axis=(0, 2))
    mass = jnp.pad(jnp.concatenate([before, after]), (0, LANES - 2 * FIELDS))
    parties = (LAT[0], LAT[1], "lev")
    spread = jnp.broadcast_to(mass[None, None], (lax.axis_size(parties), 1, LANES))
    spread = lax.all_to_all(spread, parties, 0, 0)
    mass = jnp.sum(spread, axis=(0, 1))
    ratio = mass[:FIELDS] / mass[FIELDS : 2 * FIELDS]
    lon_w = jnp.stack(cubic_weights(lon_fraction))

    result = None
    half = ROWS // 2
    for field in range(FIELDS):
        operands = [piece for chunk in field_chunks(field) for piece in gathered[chunk]]
        in_specs = [SMEM, SMEM, SMEM] + [VMEM] * len(operands)
        aliases = {}
        if result is not None:
            operands.append(result)
            in_specs.append(ANY)
            aliases = {len(in_specs) - 1: 0}
        result = pl.pallas_call(
            partial(finish_kernel, field, half),
            grid=(2,),
            out_shape=jax.ShapeDtypeStruct(fields.shape, jnp.float32),
            in_specs=in_specs,
            out_specs=pl.BlockSpec((half, 1, 8, LON), lambda i, field=field: (i, field, 0, 0)),
            scratch_shapes=[pltpu.VMEM((2 * TILES, 8, LANES), jnp.float32)],
            input_output_aliases=aliases,
            compiler_params=params,
            name="finish",
        )(lon_shift, lon_w, ratio, *operands)
    return result


def solution(mesh):
    finer = Mesh(mesh.devices.reshape(4, 8, 4, mesh.shape["lev"]), LAT + ("lev",))
    placed = (P(LAT, None, "lev", None), P(LAT), P(LAT), P(LAT), P(LAT), P(LAT, None))
    return jax.shard_map(
        per_device,
        mesh=finer,
        in_specs=placed,
        out_specs=P(LAT, None, "lev", None),
        check_vma=False,
    )
```

```python
import math
from functools import partial

import jax
import jax.numpy as jnp
from jax import lax
from jax.experimental import pallas as pl
from jax.experimental.pallas import tpu as pltpu
from jax.sharding import Mesh
from jax.sharding import PartitionSpec as P


LAT = ("lat_0", "lat_1", "lat_2")
ROWS = 10
RING = 4
GROUP = RING * ROWS
FIELDS = 3
LANES = 128
QUARTER = 5
TILES = RING * QUARTER
LON = TILES * LANES
CUTS = (0, 2, 7, 12, 15)
CHUNKS = tuple(zip(CUTS[:-1], CUTS[1:]))
INFO_CHUNK = 1
TOGETHER = 2
VMEM_LIMIT = 10 * 1024 * 1024


VMEM = pl.BlockSpec(memory_space=pltpu.VMEM)
SMEM = pl.BlockSpec(memory_space=pltpu.SMEM)
ANY = pl.BlockSpec(memory_space=pl.ANY)


def cubic_weights(fraction):
    return (
        -fraction * (fraction - 1.0) * (fraction - 2.0) / 6.0,
        (fraction + 1.0) * (fraction - 1.0) * (fraction - 2.0) / 2.0,
        -(fraction + 1.0) * fraction * (fraction - 2.0) / 2.0,
        (fraction + 1.0) * fraction * (fraction - 1.0) / 6.0,
    )


def around(place, distance):
    return lax.rem(place + RING + distance, RING)


def tile_count(chunk):
    first, last = CHUNKS[chunk]
    return ROWS * (last - first) + (1 if chunk == INFO_CHUNK else 0)


def copy_units(fields_ref, chunk, piece_refs):
    first, last = CHUNKS[chunk]
    width = last - first
    place = lax.axis_index(LAT[2])
    for distance in range(RING):
        owner = around(place, distance)
        for unit in range(first, last):
            field, tile = divmod(unit, QUARTER)
            start = pl.multiple_of((owner * QUARTER + tile) * LANES, LANES)
            for row in range(ROWS):
                piece_refs[distance][row * width + unit - first] = fields_ref[
                    row, field, :, pl.ds(start, LANES)
                ]


def pack_first(fields_ref, *piece_refs):
    copy_units(fields_ref, 0, piece_refs)


def pack_rest(departure_ref, extents_ref, lat_ref, lon_ref, fields_ref, *piece_refs):
    band = lax.axis_index(LAT)
    first_row = band * ROWS
    group_row = lax.axis_index(LAT[:2]) * GROUP
    low_bound = first_row - extents_ref[0, 0] * ROWS + 1
    high_bound = first_row + ROWS - 3 + extents_ref[0, 1] * ROWS
    info_sub = lax.broadcasted_iota(jnp.int32, (8, LANES), 0)
    info_lane = lax.broadcasted_iota(jnp.int32, (8, LANES), 1)
    starts = jnp.zeros((8, LANES), jnp.int32)
    info = jnp.zeros((8, LANES), jnp.float32)
    for row in range(ROWS):
        departure = jnp.clip(departure_ref[row], low_bound, high_bound)
        departure = jnp.clip(departure, 1, RING * 32 * ROWS - 3)
        here = info_lane == row
        starts = jnp.where(here, departure - 1 - (group_row - GROUP), starts)
        info = jnp.where(here & (info_sub == 1), lat_ref[row], info)
        info = jnp.where(here & (info_sub == 2), lon_ref[row], info)
    info = jnp.where(info_sub == 0, starts.astype(jnp.float32), info)
    sub = lax.broadcasted_iota(jnp.int32, (ROWS, LANES), 0)
    lane = lax.broadcasted_iota(jnp.int32, (ROWS, LANES), 1)
    for field in range(FIELDS):
        total = fields_ref[:, field, :, 0:LANES]
        for tile in range(1, TILES):
            total = total + fields_ref[:, field, :, tile * LANES : (tile + 1) * LANES]
        by_row = jnp.sum(jnp.sum(total, axis=1), axis=1, keepdims=True)
        in_lanes = jnp.sum(jnp.where(sub == lane, by_row, 0.0), axis=0, keepdims=True)
        info = jnp.where(info_sub == 3 + field, in_lanes, info)
    for chunk in range(1, len(CHUNKS)):
        refs = piece_refs[(chunk - 1) * RING : chunk * RING]
        copy_units(fields_ref, chunk, refs)
        if chunk == INFO_CHUNK:
            for ref in refs:
                ref[tile_count(chunk) - 1] = info


def join_kernel(*refs):
    for distance in range(RING):
        refs[RING][distance] = refs[distance][...]
        for info_ref in refs[RING + 1 :]:
            info_ref[distance] = refs[distance][tile_count(INFO_CHUNK) - 1]


def column_kernel(width, start_ref, weight_ref, north_ref, own_ref, south_ref, *refs):
    out_refs, rows_ref = refs[:RING], refs[-1]
    count = width * ROWS
    place = lax.axis_index(LAT[2])
    for info_ref in refs[RING:-1]:
        for side, ref in enumerate((north_ref, own_ref, south_ref)):
            info_ref[side] = ref[:, count]
    for distance in range(RING):
        band = around(place, -distance)
        for side, ref in enumerate((north_ref, own_ref, south_ref)):
            rows_ref[pl.ds((side * RING + band) * count, count)] = ref[distance, :count]

    def one_row(row, carry):
        for distance in range(RING):
            source = (RING - distance) % RING
            first = start_ref[source, row]
            total = weight_ref[0, source, row] * rows_ref[pl.ds(first * width, width)]
            for step in range(1, 4):
                total = total + weight_ref[step, source, row] * rows_ref[pl.ds((first + step) * width, width)]
            out_refs[distance][pl.ds(row * width, width)] = total
        return carry

    lax.fori_loop(0, ROWS, one_row, 0)


def field_units(field):
    found = []
    for tile in range(QUARTER):
        unit = field * QUARTER + tile
        for chunk, (first, last) in enumerate(CHUNKS):
            if first <= unit < last:
                found.append((chunk, unit - first, last - first))
    return found


def field_chunks(field):
    return sorted({chunk for chunk, _, _ in field_units(field)})


def finish_kernel(field, shift_ref, weight_ref, ratio_ref, *refs):
    out_ref, turned_ref = refs[-2], refs[-1]
    chunks = field_chunks(field)
    place = lax.axis_index(LAT[2])
    owners = [around(place, -distance) for distance in range(RING)]
    lane = lax.broadcasted_iota(jnp.int32, (8, LANES), 1)
    scale = ratio_ref[field]

    def ahead(values, step):
        moved = [pltpu.roll(value, LANES - step, 1) for value in values]
        following = moved[1:] + moved[:1]
        return [jnp.where(lane < LANES - step, here, then) for here, then in zip(moved, following)]

    def some_rows(pair, carry):
        for member in range(TOGETHER):
            row = pair * TOGETHER + member
            slot = member * 2 * TILES
            base = shift_ref[row]
            base = jnp.where(base == 0, LON - 1, base - 1)
            whole = base // LANES
            back = LANES - (base - whole * LANES)
            for distance in range(RING):
                for tile, (chunk, at, width) in enumerate(field_units(field)):
                    piece = refs[chunks.index(chunk) * RING + distance][row * width + at]
                    turned_ref[slot + owners[distance] * QUARTER + tile] = piece
                    turned_ref[slot + TILES + owners[distance] * QUARTER + tile] = piece
            weights = [weight_ref[step, row] * scale for step in range(4)]
            rolled = [pltpu.roll(turned_ref[slot + whole + tile], back, 1) for tile in range(TILES)]
            lined = [jnp.where(lane < back, here, then) for here, then in zip(rolled, rolled[1:] + rolled[:1])]
            next_one = ahead(lined, 1)
            far = ahead([weights[2] * here + weights[3] * then for here, then in zip(lined, next_one)], 2)
            for tile in range(TILES):
                out_ref[row, 0, :, tile * LANES : (tile + 1) * LANES] = (
                    weights[0] * lined[tile] + weights[1] * next_one[tile] + far[tile]
                )
        return carry

    lax.fori_loop(0, ROWS // TOGETHER, some_rows, 0)


def turn(array, axis, distance):
    count = lax.axis_size(axis)
    return lax.ppermute(array, axis, [(i, (i + distance) % count) for i in range(count)])


def exchange(pieces):
    return [pieces[0]] + [turn(pieces[distance], LAT[2], distance) for distance in range(1, RING)]


def tiles(*shape):
    return jax.ShapeDtypeStruct((*shape, 8, LANES), jnp.float32)


def per_device(fields, lat_fraction, lon_fraction, lon_shift, departure_row, extents):
    params = pltpu.CompilerParams(vmem_limit_bytes=VMEM_LIMIT)
    last_chunk = len(CHUNKS)

    width = CHUNKS[0][1]
    first_pieces = pl.pallas_call(
        pack_first,
        out_shape=[tiles(ROWS * width)] * RING,
        in_specs=[VMEM],
        out_specs=[VMEM] * RING,
        compiler_params=params,
        name="pack_a",
    )(fields)
    rest = pl.pallas_call(
        pack_rest,
        out_shape=[tiles(tile_count(chunk)) for chunk in range(1, last_chunk) for _ in range(RING)],
        in_specs=[SMEM] * 4 + [VMEM],
        out_specs=[VMEM] * (RING * (last_chunk - 1)),
        compiler_params=params,
        name="pack_b",
    )(departure_row, extents, lat_fraction, lon_fraction, fields)
    pieces = [first_pieces] + [rest[i * RING : (i + 1) * RING] for i in range(last_chunk - 1)]

    own, north, south = [], [], []
    for chunk in range(last_chunk):
        received = exchange(pieces[chunk])
        joined = pl.pallas_call(
            join_kernel,
            out_shape=[tiles(RING, tile_count(chunk))] + [tiles(RING)] * (chunk == INFO_CHUNK),
            in_specs=[VMEM] * RING,
            out_specs=[VMEM] * (2 if chunk == INFO_CHUNK else 1),
            compiler_params=params,
            name="join",
        )(*received)
        if chunk == INFO_CHUNK:
            ring_info = joined[1][:, :, :ROWS]
        joined = joined[0]
        north.append(turn(joined, LAT[:2], 1))
        south.append(turn(joined, LAT[:2], -1))
        own.append(joined)

    ring_start = ring_info[:, 0].astype(jnp.int32)
    ring_weight = jnp.stack(cubic_weights(ring_info[:, 1]))

    gathered = []
    for chunk, (first, last) in enumerate(CHUNKS):
        width = last - first
        columns = pl.pallas_call(
            partial(column_kernel, width),
            out_shape=[tiles(ROWS * width)] * RING + [tiles(3, RING)] * (chunk == INFO_CHUNK),
            in_specs=[SMEM, SMEM, VMEM, VMEM, VMEM],
            out_specs=[VMEM] * (RING + (chunk == INFO_CHUNK)),
            scratch_shapes=[pltpu.VMEM((3 * GROUP * width, 8, LANES), jnp.float32)],
            compiler_params=params,
            name="column",
        )(ring_start, ring_weight, north[chunk], own[chunk], south[chunk])
        if chunk == INFO_CHUNK:
            all_info = columns[RING]
        gathered.append(exchange(columns[:RING]))

    total_rows = lax.axis_size(LAT) * ROWS
    group_row = lax.axis_index(LAT[:2]) * GROUP
    bands = around(lax.axis_index(LAT[2]), -jnp.arange(RING, dtype=jnp.int32))
    ring_rows = bands[:, None] * ROWS + jnp.arange(ROWS, dtype=jnp.int32)[None]
    area = jnp.cos(math.pi * ((group_row + ring_rows).astype(jnp.float32) + 0.5) / total_rows - math.pi / 2.0)
    sums = all_info[:, :, 3 : 3 + FIELDS, :ROWS]
    lon_total = sum(cubic_weights(ring_info[:, 2]))
    before = jnp.sum(area[:, None, :] * sums[1], axis=(0, 2))
    after = jnp.zeros((FIELDS,), jnp.float32)
    for side in range(3):
        spots = side * GROUP + ring_rows
        factor = jnp.zeros((RING, ROWS), jnp.float32)
        for step in range(4):
            hit = (ring_start + step)[None, None] == spots[..., None, None]
            share = area * lon_total * ring_weight[step]
            factor = factor + jnp.sum(jnp.where(hit, share[None, None], 0.0), axis=(2, 3))
        after = after + jnp.sum(factor[:, None, :] * sums[side], axis=(0, 2))
    mass = jnp.pad(jnp.concatenate([before, after]), (0, LANES - 2 * FIELDS))
    parties = (LAT[0], LAT[1], "lev")
    spread = jnp.broadcast_to(mass[None, None], (lax.axis_size(parties), 1, LANES))
    spread = lax.all_to_all(spread, parties, 0, 0)
    mass = jnp.sum(spread, axis=(0, 1))
    ratio = mass[:FIELDS] / mass[FIELDS : 2 * FIELDS]
    lon_w = jnp.stack(cubic_weights(lon_fraction))

    result = None
    for field in range(FIELDS):
        operands = [piece for chunk in field_chunks(field) for piece in gathered[chunk]]
        in_specs = [SMEM, SMEM, SMEM] + [VMEM] * len(operands)
        aliases = {}
        if result is not None:
            operands.append(result)
            in_specs.append(ANY)
            aliases = {len(in_specs) - 1: 0}
        result = pl.pallas_call(
            partial(finish_kernel, field),
            grid=(1,),
            out_shape=jax.ShapeDtypeStruct(fields.shape, jnp.float32),
            in_specs=in_specs,
            out_specs=pl.BlockSpec((ROWS, 1, 8, LON), lambda i, field=field: (0, field, 0, 0)),
            scratch_shapes=[pltpu.VMEM((TOGETHER * 2 * TILES, 8, LANES), jnp.float32)],
            input_output_aliases=aliases,
            compiler_params=params,
            name="finish",
        )(lon_shift, lon_w, ratio, *operands)
    return result


def solution(mesh):
    finer = Mesh(mesh.devices.reshape(4, 8, 4, mesh.shape["lev"]), LAT + ("lev",))
    placed = (P(LAT, None, "lev", None), P(LAT), P(LAT), P(LAT), P(LAT), P(LAT, None))
    return jax.shard_map(
        per_device,
        mesh=finer,
        in_specs=placed,
        out_specs=P(LAT, None, "lev", None),
        check_vma=False,
    )
```

```python
import math
from functools import partial

import jax
import jax.numpy as jnp
from jax import lax
from jax.experimental import pallas as pl
from jax.experimental.pallas import tpu as pltpu
from jax.sharding import Mesh
from jax.sharding import PartitionSpec as P


LAT = ("lat_0", "lat_1", "lat_2")
ROWS = 10
RING = 4
GROUP = RING * ROWS
FIELDS = 3
LANES = 128
QUARTER = 5
TILES = RING * QUARTER
LON = TILES * LANES
CHUNKS = ((0, 2), (2, 8), (8, 13), (13, 15))
OWN = ((0,), (1,), (2, 3))
BACK = ((0, 1), (2,), (3,))
INFO_CHUNK = 1
TOGETHER = 2
VMEM_LIMIT = 12 * 1024 * 1024


VMEM = pl.BlockSpec(memory_space=pltpu.VMEM)
SMEM = pl.BlockSpec(memory_space=pltpu.SMEM)
ANY = pl.BlockSpec(memory_space=pl.ANY)


def cubic_weights(fraction):
    return (
        -fraction * (fraction - 1.0) * (fraction - 2.0) / 6.0,
        (fraction + 1.0) * (fraction - 1.0) * (fraction - 2.0) / 2.0,
        -(fraction + 1.0) * fraction * (fraction - 2.0) / 2.0,
        (fraction + 1.0) * fraction * (fraction - 1.0) / 6.0,
    )


def around(place, distance):
    return lax.rem(place + RING + distance, RING)


def width_of(chunk):
    first, last = CHUNKS[chunk]
    return last - first


def tile_count(chunk):
    return ROWS * width_of(chunk) + (1 if chunk == INFO_CHUNK else 0)


def batch_tiles(batch):
    return sum(tile_count(chunk) for chunk in batch)


def column_tiles(batch):
    return sum(ROWS * width_of(chunk) for chunk in batch)


def copy_units(fields_ref, batch, piece_refs):
    place = lax.axis_index(LAT[2])
    for distance in range(RING):
        owner = around(place, distance)
        base = 0
        for chunk in batch:
            first, last = CHUNKS[chunk]
            for unit in range(first, last):
                field, tile = divmod(unit, QUARTER)
                start = pl.multiple_of((owner * QUARTER + tile) * LANES, LANES)
                for row in range(ROWS):
                    piece_refs[distance][base + row * (last - first) + unit - first] = fields_ref[
                        row, field, :, pl.ds(start, LANES)
                    ]
            base += tile_count(chunk)


def pack_first(fields_ref, *piece_refs):
    copy_units(fields_ref, OWN[0], piece_refs)


def pack_rest(departure_ref, extents_ref, lat_ref, lon_ref, fields_ref, *piece_refs):
    band = lax.axis_index(LAT)
    first_row = band * ROWS
    group_row = lax.axis_index(LAT[:2]) * GROUP
    low_bound = first_row - extents_ref[0, 0] * ROWS + 1
    high_bound = first_row + ROWS - 3 + extents_ref[0, 1] * ROWS
    info_sub = lax.broadcasted_iota(jnp.int32, (8, LANES), 0)
    info_lane = lax.broadcasted_iota(jnp.int32, (8, LANES), 1)
    starts = jnp.zeros((8, LANES), jnp.int32)
    info = jnp.zeros((8, LANES), jnp.float32)
    for row in range(ROWS):
        departure = jnp.clip(departure_ref[row], low_bound, high_bound)
        departure = jnp.clip(departure, 1, RING * 32 * ROWS - 3)
        here = info_lane == row
        starts = jnp.where(here, departure - 1 - (group_row - GROUP), starts)
        info = jnp.where(here & (info_sub == 1), lat_ref[row], info)
        info = jnp.where(here & (info_sub == 2), lon_ref[row], info)
    info = jnp.where(info_sub == 0, starts.astype(jnp.float32), info)
    sub = lax.broadcasted_iota(jnp.int32, (ROWS, LANES), 0)
    lane = lax.broadcasted_iota(jnp.int32, (ROWS, LANES), 1)
    for field in range(FIELDS):
        total = fields_ref[:, field, :, 0:LANES]
        for tile in range(1, TILES):
            total = total + fields_ref[:, field, :, tile * LANES : (tile + 1) * LANES]
        by_row = jnp.sum(jnp.sum(total, axis=1), axis=1, keepdims=True)
        in_lanes = jnp.sum(jnp.where(sub == lane, by_row, 0.0), axis=0, keepdims=True)
        info = jnp.where(info_sub == 3 + field, in_lanes, info)
    for number, batch in enumerate(OWN[1:]):
        refs = piece_refs[number * RING : (number + 1) * RING]
        copy_units(fields_ref, batch, refs)
        if INFO_CHUNK in batch:
            for ref in refs:
                ref[batch_tiles(batch) - 1] = info


def join_kernel(batch, *refs):
    out_refs = refs[RING:]
    for distance in range(RING):
        base = 0
        for out_ref, chunk in zip(out_refs, batch):
            out_ref[distance] = refs[distance][base : base + tile_count(chunk)]
            base += tile_count(chunk)
        if INFO_CHUNK in batch:
            out_refs[-1][distance] = refs[distance][batch_tiles(batch) - 1]


def column_kernel(batch, start_ref, weight_ref, *refs):
    sides = [refs[3 * number : 3 * number + 3] for number in range(len(batch))]
    refs = refs[3 * len(batch) :]
    out_refs, rows_refs = refs[:RING], refs[len(refs) - len(batch) :]
    place = lax.axis_index(LAT[2])
    for chunk, side_refs, rows_ref in zip(batch, sides, rows_refs):
        count = width_of(chunk) * ROWS
        if chunk == INFO_CHUNK:
            for side, ref in enumerate(side_refs):
                refs[RING][side] = ref[:, count]
        for distance in range(RING):
            band = around(place, -distance)
            for side, ref in enumerate(side_refs):
                rows_ref[pl.ds((side * RING + band) * count, count)] = ref[distance, :count]

    def one_row(row, carry):
        for distance in range(RING):
            source = (RING - distance) % RING
            first = start_ref[source, row]
            weights = [weight_ref[step, source, row] for step in range(4)]
            base = 0
            for chunk, rows_ref in zip(batch, rows_refs):
                width = width_of(chunk)
                total = weights[0] * rows_ref[pl.ds(first * width, width)]
                for step in range(1, 4):
                    total = total + weights[step] * rows_ref[pl.ds((first + step) * width, width)]
                out_refs[distance][pl.ds(base + row * width, width)] = total
                base += ROWS * width
        return carry

    lax.fori_loop(0, ROWS, one_row, 0)


def field_units(field):
    found = []
    for tile in range(QUARTER):
        unit = field * QUARTER + tile
        for number, batch in enumerate(BACK):
            base = 0
            for chunk in batch:
                first, last = CHUNKS[chunk]
                if first <= unit < last:
                    found.append((number, base + unit - first, last - first))
                base += ROWS * (last - first)
    return found


def field_batches(field):
    return sorted({number for number, _, _ in field_units(field)})


def finish_kernel(field, shift_ref, weight_ref, ratio_ref, *refs):
    out_ref, turned_ref = refs[-2], refs[-1]
    batches = field_batches(field)
    place = lax.axis_index(LAT[2])
    owners = [around(place, -distance) for distance in range(RING)]
    lane = lax.broadcasted_iota(jnp.int32, (8, LANES), 1)
    scale = ratio_ref[field]

    def ahead(values, step):
        moved = [pltpu.roll(value, LANES - step, 1) for value in values]
        following = moved[1:] + moved[:1]
        return [jnp.where(lane < LANES - step, here, then) for here, then in zip(moved, following)]

    def some_rows(pair, carry):
        for member in range(TOGETHER):
            row = pair * TOGETHER + member
            slot = member * 2 * TILES
            base = shift_ref[row]
            base = jnp.where(base == 0, LON - 1, base - 1)
            whole = base // LANES
            back = LANES - (base - whole * LANES)
            for distance in range(RING):
                for tile, (number, at, width) in enumerate(field_units(field)):
                    piece = refs[batches.index(number) * RING + distance][row * width + at]
                    turned_ref[slot + owners[distance] * QUARTER + tile] = piece
                    turned_ref[slot + TILES + owners[distance] * QUARTER + tile] = piece
            weights = [weight_ref[step, row] * scale for step in range(4)]
            rolled = [pltpu.roll(turned_ref[slot + whole + tile], back, 1) for tile in range(TILES)]
            lined = [jnp.where(lane < back, here, then) for here, then in zip(rolled, rolled[1:] + rolled[:1])]
            next_one = ahead(lined, 1)
            far = ahead([weights[2] * here + weights[3] * then for here, then in zip(lined, next_one)], 2)
            for tile in range(TILES):
                out_ref[row, 0, :, tile * LANES : (tile + 1) * LANES] = (
                    weights[0] * lined[tile] + weights[1] * next_one[tile] + far[tile]
                )
        return carry

    lax.fori_loop(0, ROWS // TOGETHER, some_rows, 0)


def turn(array, axis, distance):
    count = lax.axis_size(axis)
    return lax.ppermute(array, axis, [(i, (i + distance) % count) for i in range(count)])


def exchange(pieces):
    return [pieces[0]] + [turn(pieces[distance], LAT[2], distance) for distance in range(1, RING)]


def tiles(*shape):
    return jax.ShapeDtypeStruct((*shape, 8, LANES), jnp.float32)


def per_device(fields, lat_fraction, lon_fraction, lon_shift, departure_row, extents):
    params = pltpu.CompilerParams(vmem_limit_bytes=VMEM_LIMIT)
    pieces = [
        pl.pallas_call(
            pack_first,
            out_shape=[tiles(batch_tiles(OWN[0]))] * RING,
            in_specs=[VMEM],
            out_specs=[VMEM] * RING,
            compiler_params=params,
            name="pack_a",
        )(fields)
    ]
    rest = pl.pallas_call(
        pack_rest,
        out_shape=[tiles(batch_tiles(batch)) for batch in OWN[1:] for _ in range(RING)],
        in_specs=[SMEM] * 4 + [VMEM],
        out_specs=[VMEM] * (RING * (len(OWN) - 1)),
        compiler_params=params,
        name="pack_b",
    )(departure_row, extents, lat_fraction, lon_fraction, fields)
    pieces += [rest[number * RING : (number + 1) * RING] for number in range(len(OWN) - 1)]

    own, north, south = {}, {}, {}
    for number, batch in enumerate(OWN):
        received = exchange(pieces[number])
        shapes = [tiles(RING, tile_count(chunk)) for chunk in batch] + [tiles(RING)] * (INFO_CHUNK in batch)
        joined = pl.pallas_call(
            partial(join_kernel, batch),
            out_shape=shapes,
            in_specs=[VMEM] * RING,
            out_specs=[VMEM] * len(shapes),
            compiler_params=params,
            name="join",
        )(*received)
        if INFO_CHUNK in batch:
            ring_info = joined[-1][:, :, :ROWS]
        for chunk, block in zip(batch, joined):
            own[chunk] = block
            north[chunk] = turn(block, LAT[:2], 1)
            south[chunk] = turn(block, LAT[:2], -1)

    ring_start = ring_info[:, 0].astype(jnp.int32)
    ring_weight = jnp.stack(cubic_weights(ring_info[:, 1]))

    gathered = []
    for batch in BACK:
        shapes = [tiles(column_tiles(batch))] * RING + [tiles(3, RING)] * (INFO_CHUNK in batch)
        operands = [part[chunk] for chunk in batch for part in (north, own, south)]
        columns = pl.pallas_call(
            partial(column_kernel, batch),
            out_shape=shapes,
            in_specs=[SMEM, SMEM] + [VMEM] * len(operands),
            out_specs=[VMEM] * len(shapes),
            scratch_shapes=[
                pltpu.VMEM((3 * GROUP * width_of(chunk), 8, LANES), jnp.float32) for chunk in batch
            ],
            compiler_params=params,
            name="column",
        )(ring_start, ring_weight, *operands)
        if INFO_CHUNK in batch:
            all_info = columns[RING]
        gathered.append(exchange(columns[:RING]))

    total_rows = lax.axis_size(LAT) * ROWS
    group_row = lax.axis_index(LAT[:2]) * GROUP
    bands = around(lax.axis_index(LAT[2]), -jnp.arange(RING, dtype=jnp.int32))
    ring_rows = bands[:, None] * ROWS + jnp.arange(ROWS, dtype=jnp.int32)[None]
    area = jnp.cos(math.pi * ((group_row + ring_rows).astype(jnp.float32) + 0.5) / total_rows - math.pi / 2.0)
    sums = all_info[:, :, 3 : 3 + FIELDS, :ROWS]
    lon_total = sum(cubic_weights(ring_info[:, 2]))
    before = jnp.sum(area[:, None, :] * sums[1], axis=(0, 2))
    after = jnp.zeros((FIELDS,), jnp.float32)
    for side in range(3):
        spots = side * GROUP + ring_rows
        factor = jnp.zeros((RING, ROWS), jnp.float32)
        for step in range(4):
            hit = (ring_start + step)[None, None] == spots[..., None, None]
            share = area * lon_total * ring_weight[step]
            factor = factor + jnp.sum(jnp.where(hit, share[None, None], 0.0), axis=(2, 3))
        after = after + jnp.sum(factor[:, None, :] * sums[side], axis=(0, 2))
    mass = jnp.pad(jnp.concatenate([before, after]), (0, LANES - 2 * FIELDS))
    parties = (LAT[0], LAT[1], "lev")
    spread = jnp.broadcast_to(mass[None, None], (lax.axis_size(parties), 1, LANES))
    spread = lax.all_to_all(spread, parties, 0, 0)
    mass = jnp.sum(spread, axis=(0, 1))
    ratio = mass[:FIELDS] / mass[FIELDS : 2 * FIELDS]
    lon_w = jnp.stack(cubic_weights(lon_fraction))

    result = None
    for field in range(FIELDS):
        operands = [piece for number in field_batches(field) for piece in gathered[number]]
        in_specs = [SMEM, SMEM, SMEM] + [VMEM] * len(operands)
        aliases = {}
        if result is not None:
            operands.append(result)
            in_specs.append(ANY)
            aliases = {len(in_specs) - 1: 0}
        result = pl.pallas_call(
            partial(finish_kernel, field),
            grid=(1,),
            out_shape=jax.ShapeDtypeStruct(fields.shape, jnp.float32),
            in_specs=in_specs,
            out_specs=pl.BlockSpec((ROWS, 1, 8, LON), lambda i, field=field: (0, field, 0, 0)),
            scratch_shapes=[pltpu.VMEM((TOGETHER * 2 * TILES, 8, LANES), jnp.float32)],
            input_output_aliases=aliases,
            compiler_params=params,
            name="finish",
        )(lon_shift, lon_w, ratio, *operands)
    return result


def solution(mesh):
    finer = Mesh(mesh.devices.reshape(4, 8, 4, mesh.shape["lev"]), LAT + ("lev",))
    placed = (P(LAT, None, "lev", None), P(LAT), P(LAT), P(LAT), P(LAT), P(LAT, None))
    return jax.shard_map(
        per_device,
        mesh=finer,
        in_specs=placed,
        out_specs=P(LAT, None, "lev", None),
        check_vma=False,
    )
```

```python
import math
from functools import partial

import jax
import jax.numpy as jnp
from jax import lax
from jax.experimental import pallas as pl
from jax.experimental.pallas import tpu as pltpu
from jax.sharding import Mesh
from jax.sharding import PartitionSpec as P


LAT = ("lat_0", "lat_1", "lat_2")
ROWS = 10
RING = 4
GROUP = RING * ROWS
FIELDS = 3
LANES = 128
QUARTER = 5
TILES = RING * QUARTER
LON = TILES * LANES
CHUNKS = ((0, 2), (2, 8), (8, 13), (13, 15))
EARLY = 0
OWN = ((1,), (2, 3))
BACK = ((0, 1), (2,), (3,))
INFO_CHUNK = 1
TOGETHER = 2
VMEM_LIMIT = 12 * 1024 * 1024


VMEM = pl.BlockSpec(memory_space=pltpu.VMEM)
SMEM = pl.BlockSpec(memory_space=pltpu.SMEM)
ANY = pl.BlockSpec(memory_space=pl.ANY)


def cubic_weights(fraction):
    return (
        -fraction * (fraction - 1.0) * (fraction - 2.0) / 6.0,
        (fraction + 1.0) * (fraction - 1.0) * (fraction - 2.0) / 2.0,
        -(fraction + 1.0) * fraction * (fraction - 2.0) / 2.0,
        (fraction + 1.0) * fraction * (fraction - 1.0) / 6.0,
    )


def around(place, distance):
    return lax.rem(place + RING + distance, RING)


def width_of(chunk):
    first, last = CHUNKS[chunk]
    return last - first


def tile_count(chunk):
    return ROWS * width_of(chunk) + (1 if chunk == INFO_CHUNK else 0)


def batch_tiles(batch):
    return sum(tile_count(chunk) for chunk in batch)


def column_tiles(batch):
    return sum(ROWS * width_of(chunk) for chunk in batch)


def copy_units(fields_ref, chunk, owner, piece_ref, base):
    first, last = CHUNKS[chunk]
    for unit in range(first, last):
        field, tile = divmod(unit, QUARTER)
        start = pl.multiple_of((owner * QUARTER + tile) * LANES, LANES)
        for row in range(ROWS):
            piece_ref[base + row * (last - first) + unit - first] = fields_ref[row, field, :, pl.ds(start, LANES)]


def pack_kernel(departure_ref, extents_ref, lat_ref, lon_ref, fields_ref, early_ref, *piece_refs):
    band = lax.axis_index(LAT)
    place = lax.axis_index(LAT[2])
    first_row = band * ROWS
    group_row = lax.axis_index(LAT[:2]) * GROUP
    low_bound = first_row - extents_ref[0, 0] * ROWS + 1
    high_bound = first_row + ROWS - 3 + extents_ref[0, 1] * ROWS
    info_sub = lax.broadcasted_iota(jnp.int32, (8, LANES), 0)
    info_lane = lax.broadcasted_iota(jnp.int32, (8, LANES), 1)
    starts = jnp.zeros((8, LANES), jnp.int32)
    info = jnp.zeros((8, LANES), jnp.float32)
    for row in range(ROWS):
        departure = jnp.clip(departure_ref[row], low_bound, high_bound)
        departure = jnp.clip(departure, 1, RING * 32 * ROWS - 3)
        here = info_lane == row
        starts = jnp.where(here, departure - 1 - (group_row - GROUP), starts)
        info = jnp.where(here & (info_sub == 1), lat_ref[row], info)
        info = jnp.where(here & (info_sub == 2), lon_ref[row], info)
    info = jnp.where(info_sub == 0, starts.astype(jnp.float32), info)
    sub = lax.broadcasted_iota(jnp.int32, (ROWS, LANES), 0)
    lane = lax.broadcasted_iota(jnp.int32, (ROWS, LANES), 1)
    for field in range(FIELDS):
        total = fields_ref[:, field, :, 0:LANES]
        for tile in range(1, TILES):
            total = total + fields_ref[:, field, :, tile * LANES : (tile + 1) * LANES]
        by_row = jnp.sum(jnp.sum(total, axis=1), axis=1, keepdims=True)
        in_lanes = jnp.sum(jnp.where(sub == lane, by_row, 0.0), axis=0, keepdims=True)
        info = jnp.where(info_sub == 3 + field, in_lanes, info)
    for distance in range(RING):
        owner = around(place, distance)
        copy_units(fields_ref, EARLY, owner, early_ref.at[distance], 0)
        for number, batch in enumerate(OWN):
            piece_ref = piece_refs[number * RING + distance]
            base = 0
            for chunk in batch:
                copy_units(fields_ref, chunk, owner, piece_ref, base)
                base += tile_count(chunk)
            if INFO_CHUNK in batch:
                piece_ref[base - 1] = info


def bundle_kernel(north_ref, own_ref, south_ref, *out_refs):
    count = tile_count(EARLY)
    for distance in range(RING):
        for side, ref in enumerate((north_ref, own_ref, south_ref)):
            out_refs[distance][side * count : (side + 1) * count] = ref[distance]


def join_kernel(batch, *refs):
    out_refs = refs[RING:]
    for distance in range(RING):
        base = 0
        for out_ref, chunk in zip(out_refs, batch):
            out_ref[distance] = refs[distance][base : base + tile_count(chunk)]
            base += tile_count(chunk)
        if INFO_CHUNK in batch:
            out_refs[-1][distance] = refs[distance][batch_tiles(batch) - 1]


def column_kernel(batch, start_ref, weight_ref, *refs):
    sides = []
    for chunk in batch:
        taken = RING if chunk == EARLY else 3
        sides.append(refs[:taken])
        refs = refs[taken:]
    out_refs, rows_refs = refs[:RING], refs[len(refs) - len(batch) :]
    place = lax.axis_index(LAT[2])
    for chunk, side_refs, rows_ref in zip(batch, sides, rows_refs):
        count = width_of(chunk) * ROWS
        if chunk == INFO_CHUNK:
            for side, ref in enumerate(side_refs):
                refs[RING][side] = ref[:, count]
        for distance in range(RING):
            band = around(place, -distance)
            for side in range(3):
                if chunk == EARLY:
                    block = side_refs[distance][side * count : (side + 1) * count]
                else:
                    block = side_refs[side][distance, :count]
                rows_ref[pl.ds((side * RING + band) * count, count)] = block

    def one_row(row, carry):
        for distance in range(RING):
            source = (RING - distance) % RING
            first = start_ref[source, row]
            weights = [weight_ref[step, source, row] for step in range(4)]
            base = 0
            for chunk, rows_ref in zip(batch, rows_refs):
                width = width_of(chunk)
                total = weights[0] * rows_ref[pl.ds(first * width, width)]
                for step in range(1, 4):
                    total = total + weights[step] * rows_ref[pl.ds((first + step) * width, width)]
                out_refs[distance][pl.ds(base + row * width, width)] = total
                base += ROWS * width
        return carry

    lax.fori_loop(0, ROWS, one_row, 0)


def field_units(field):
    found = []
    for tile in range(QUARTER):
        unit = field * QUARTER + tile
        for number, batch in enumerate(BACK):
            base = 0
            for chunk in batch:
                first, last = CHUNKS[chunk]
                if first <= unit < last:
                    found.append((number, base + unit - first, last - first))
                base += ROWS * (last - first)
    return found


def field_batches(field):
    return sorted({number for number, _, _ in field_units(field)})


def finish_kernel(field, shift_ref, weight_ref, ratio_ref, *refs):
    out_ref, turned_ref = refs[-2], refs[-1]
    batches = field_batches(field)
    place = lax.axis_index(LAT[2])
    owners = [around(place, -distance) for distance in range(RING)]
    lane = lax.broadcasted_iota(jnp.int32, (8, LANES), 1)
    scale = ratio_ref[field]

    def ahead(values, step):
        moved = [pltpu.roll(value, LANES - step, 1) for value in values]
        following = moved[1:] + moved[:1]
        return [jnp.where(lane < LANES - step, here, then) for here, then in zip(moved, following)]

    def some_rows(pair, carry):
        for member in range(TOGETHER):
            row = pair * TOGETHER + member
            slot = member * 2 * TILES
            base = shift_ref[row]
            base = jnp.where(base == 0, LON - 1, base - 1)
            whole = base // LANES
            back = LANES - (base - whole * LANES)
            for distance in range(RING):
                for tile, (number, at, width) in enumerate(field_units(field)):
                    piece = refs[batches.index(number) * RING + distance][row * width + at]
                    turned_ref[slot + owners[distance] * QUARTER + tile] = piece
                    turned_ref[slot + TILES + owners[distance] * QUARTER + tile] = piece
            weights = [weight_ref[step, row] * scale for step in range(4)]
            rolled = [pltpu.roll(turned_ref[slot + whole + tile], back, 1) for tile in range(TILES)]
            lined = [jnp.where(lane < back, here, then) for here, then in zip(rolled, rolled[1:] + rolled[:1])]
            next_one = ahead(lined, 1)
            far = ahead([weights[2] * here + weights[3] * then for here, then in zip(lined, next_one)], 2)
            for tile in range(TILES):
                out_ref[row, 0, :, tile * LANES : (tile + 1) * LANES] = (
                    weights[0] * lined[tile] + weights[1] * next_one[tile] + far[tile]
                )
        return carry

    lax.fori_loop(0, ROWS // TOGETHER, some_rows, 0)


def turn(array, axis, distance):
    count = lax.axis_size(axis)
    return lax.ppermute(array, axis, [(i, (i + distance) % count) for i in range(count)])


def exchange(pieces):
    return [pieces[0]] + [turn(pieces[distance], LAT[2], distance) for distance in range(1, RING)]


def tiles(*shape):
    return jax.ShapeDtypeStruct((*shape, 8, LANES), jnp.float32)


def per_device(fields, lat_fraction, lon_fraction, lon_shift, departure_row, extents):
    params = pltpu.CompilerParams(vmem_limit_bytes=VMEM_LIMIT)
    early, *rest = pl.pallas_call(
        pack_kernel,
        out_shape=[tiles(RING, tile_count(EARLY))]
        + [tiles(batch_tiles(batch)) for batch in OWN for _ in range(RING)],
        in_specs=[SMEM] * 4 + [VMEM],
        out_specs=[VMEM] * (1 + RING * len(OWN)),
        compiler_params=params,
        name="pack",
    )(departure_row, extents, lat_fraction, lon_fraction, fields)
    pieces = [rest[number * RING : (number + 1) * RING] for number in range(len(OWN))]
    early_north = turn(early, LAT[:2], 1)
    early_south = turn(early, LAT[:2], -1)
    bundles = pl.pallas_call(
        bundle_kernel,
        out_shape=[tiles(3 * tile_count(EARLY))] * RING,
        in_specs=[VMEM] * 3,
        out_specs=[VMEM] * RING,
        compiler_params=params,
        name="bundle",
    )(early_north, early, early_south)
    bundles = exchange(bundles)

    own, north, south = {}, {}, {}
    for number, batch in enumerate(OWN):
        received = exchange(pieces[number])
        shapes = [tiles(RING, tile_count(chunk)) for chunk in batch] + [tiles(RING)] * (INFO_CHUNK in batch)
        joined = pl.pallas_call(
            partial(join_kernel, batch),
            out_shape=shapes,
            in_specs=[VMEM] * RING,
            out_specs=[VMEM] * len(shapes),
            compiler_params=params,
            name="join",
        )(*received)
        if INFO_CHUNK in batch:
            ring_info = joined[-1][:, :, :ROWS]
        for chunk, block in zip(batch, joined):
            own[chunk] = block
            north[chunk] = turn(block, LAT[:2], 1)
            south[chunk] = turn(block, LAT[:2], -1)

    ring_start = ring_info[:, 0].astype(jnp.int32)
    ring_weight = jnp.stack(cubic_weights(ring_info[:, 1]))

    gathered = []
    for batch in BACK:
        shapes = [tiles(column_tiles(batch))] * RING + [tiles(3, RING)] * (INFO_CHUNK in batch)
        operands = []
        for chunk in batch:
            operands += bundles if chunk == EARLY else [north[chunk], own[chunk], south[chunk]]
        columns = pl.pallas_call(
            partial(column_kernel, batch),
            out_shape=shapes,
            in_specs=[SMEM, SMEM] + [VMEM] * len(operands),
            out_specs=[VMEM] * len(shapes),
            scratch_shapes=[
                pltpu.VMEM((3 * GROUP * width_of(chunk), 8, LANES), jnp.float32) for chunk in batch
            ],
            compiler_params=params,
            name="column",
        )(ring_start, ring_weight, *operands)
        if INFO_CHUNK in batch:
            all_info = columns[RING]
        gathered.append(exchange(columns[:RING]))

    total_rows = lax.axis_size(LAT) * ROWS
    group_row = lax.axis_index(LAT[:2]) * GROUP
    bands = around(lax.axis_index(LAT[2]), -jnp.arange(RING, dtype=jnp.int32))
    ring_rows = bands[:, None] * ROWS + jnp.arange(ROWS, dtype=jnp.int32)[None]
    area = jnp.cos(math.pi * ((group_row + ring_rows).astype(jnp.float32) + 0.5) / total_rows - math.pi / 2.0)
    sums = all_info[:, :, 3 : 3 + FIELDS, :ROWS]
    lon_total = sum(cubic_weights(ring_info[:, 2]))
    before = jnp.sum(area[:, None, :] * sums[1], axis=(0, 2))
    after = jnp.zeros((FIELDS,), jnp.float32)
    for side in range(3):
        spots = side * GROUP + ring_rows
        factor = jnp.zeros((RING, ROWS), jnp.float32)
        for step in range(4):
            hit = (ring_start + step)[None, None] == spots[..., None, None]
            share = area * lon_total * ring_weight[step]
            factor = factor + jnp.sum(jnp.where(hit, share[None, None], 0.0), axis=(2, 3))
        after = after + jnp.sum(factor[:, None, :] * sums[side], axis=(0, 2))
    mass = jnp.pad(jnp.concatenate([before, after]), (0, LANES - 2 * FIELDS))
    parties = (LAT[0], LAT[1], "lev")
    spread = jnp.broadcast_to(mass[None, None], (lax.axis_size(parties), 1, LANES))
    spread = lax.all_to_all(spread, parties, 0, 0)
    mass = jnp.sum(spread, axis=(0, 1))
    ratio = mass[:FIELDS] / mass[FIELDS : 2 * FIELDS]
    lon_w = jnp.stack(cubic_weights(lon_fraction))

    result = None
    for field in range(FIELDS):
        operands = [piece for number in field_batches(field) for piece in gathered[number]]
        in_specs = [SMEM, SMEM, SMEM] + [VMEM] * len(operands)
        aliases = {}
        if result is not None:
            operands.append(result)
            in_specs.append(ANY)
            aliases = {len(in_specs) - 1: 0}
        result = pl.pallas_call(
            partial(finish_kernel, field),
            grid=(1,),
            out_shape=jax.ShapeDtypeStruct(fields.shape, jnp.float32),
            in_specs=in_specs,
            out_specs=pl.BlockSpec((ROWS, 1, 8, LON), lambda i, field=field: (0, field, 0, 0)),
            scratch_shapes=[pltpu.VMEM((TOGETHER * 2 * TILES, 8, LANES), jnp.float32)],
            input_output_aliases=aliases,
            compiler_params=params,
            name="finish",
        )(lon_shift, lon_w, ratio, *operands)
    return result


def solution(mesh):
    finer = Mesh(mesh.devices.reshape(4, 8, 4, mesh.shape["lev"]), LAT + ("lev",))
    placed = (P(LAT, None, "lev", None), P(LAT), P(LAT), P(LAT), P(LAT), P(LAT, None))
    return jax.shard_map(
        per_device,
        mesh=finer,
        in_specs=placed,
        out_specs=P(LAT, None, "lev", None),
        check_vma=False,
    )
```

```python
import math
from functools import partial

import jax
import jax.numpy as jnp
from jax import lax
from jax.experimental import pallas as pl
from jax.experimental.pallas import tpu as pltpu
from jax.sharding import Mesh
from jax.sharding import PartitionSpec as P


LAT = ("lat_0", "lat_1", "lat_2")
ROWS = 10
RING = 4
GROUP = RING * ROWS
FIELDS = 3
LANES = 128
QUARTER = 5
TILES = RING * QUARTER
LON = TILES * LANES
CHUNKS = ((0, 3), (3, 9), (9, 13), (13, 15))
PARTNERS = (2, 1, 3)
OWN = ((0,), (1,), (2, 3))
BACK = ((0, 1), (2,), (3,))
INFO_CHUNK = 1
TOGETHER = 2
VMEM_LIMIT = 12 * 1024 * 1024


VMEM = pl.BlockSpec(memory_space=pltpu.VMEM)
SMEM = pl.BlockSpec(memory_space=pltpu.SMEM)
ANY = pl.BlockSpec(memory_space=pl.ANY)


def cubic_weights(fraction):
    return (
        -fraction * (fraction - 1.0) * (fraction - 2.0) / 6.0,
        (fraction + 1.0) * (fraction - 1.0) * (fraction - 2.0) / 2.0,
        -(fraction + 1.0) * fraction * (fraction - 2.0) / 2.0,
        (fraction + 1.0) * fraction * (fraction - 1.0) / 6.0,
    )


def across(place, step):
    return jnp.bitwise_xor(place, step)


def side_places(group):
    even = 1 - lax.rem(group, 2)
    return 2 * even, 1, 2 - 2 * even


def width_of(chunk):
    first, last = CHUNKS[chunk]
    return last - first


def tile_count(chunk):
    return ROWS * width_of(chunk) + (1 if chunk == INFO_CHUNK else 0)


def batch_tiles(batch):
    return sum(tile_count(chunk) for chunk in batch)


def column_tiles(batch):
    return sum(ROWS * width_of(chunk) for chunk in batch)


def copy_units(fields_ref, batch, piece_refs):
    place = lax.axis_index(LAT[2])
    for distance in range(RING):
        owner = across(place, distance)
        base = 0
        for chunk in batch:
            first, last = CHUNKS[chunk]
            for unit in range(first, last):
                field, tile = divmod(unit, QUARTER)
                start = pl.multiple_of((owner * QUARTER + tile) * LANES, LANES)
                for row in range(ROWS):
                    piece_refs[distance][base + row * (last - first) + unit - first] = fields_ref[
                        row, field, :, pl.ds(start, LANES)
                    ]
            base += tile_count(chunk)


def pack_first(fields_ref, *piece_refs):
    copy_units(fields_ref, OWN[0], piece_refs)


def pack_rest(departure_ref, extents_ref, lat_ref, lon_ref, fields_ref, *piece_refs):
    band = lax.axis_index(LAT)
    first_row = band * ROWS
    group_row = lax.axis_index(LAT[:2]) * GROUP
    low_bound = first_row - extents_ref[0, 0] * ROWS + 1
    high_bound = first_row + ROWS - 3 + extents_ref[0, 1] * ROWS
    info_sub = lax.broadcasted_iota(jnp.int32, (8, LANES), 0)
    info_lane = lax.broadcasted_iota(jnp.int32, (8, LANES), 1)
    starts = jnp.zeros((8, LANES), jnp.int32)
    info = jnp.zeros((8, LANES), jnp.float32)
    for row in range(ROWS):
        departure = jnp.clip(departure_ref[row], low_bound, high_bound)
        departure = jnp.clip(departure, 1, RING * 32 * ROWS - 3)
        here = info_lane == row
        starts = jnp.where(here, departure - 1 - (group_row - GROUP), starts)
        info = jnp.where(here & (info_sub == 1), lat_ref[row], info)
        info = jnp.where(here & (info_sub == 2), lon_ref[row], info)
    info = jnp.where(info_sub == 0, starts.astype(jnp.float32), info)
    sub = lax.broadcasted_iota(jnp.int32, (ROWS, LANES), 0)
    lane = lax.broadcasted_iota(jnp.int32, (ROWS, LANES), 1)
    for field in range(FIELDS):
        total = fields_ref[:, field, :, 0:LANES]
        for tile in range(1, TILES):
            total = total + fields_ref[:, field, :, tile * LANES : (tile + 1) * LANES]
        by_row = jnp.sum(jnp.sum(total, axis=1), axis=1, keepdims=True)
        in_lanes = jnp.sum(jnp.where(sub == lane, by_row, 0.0), axis=0, keepdims=True)
        info = jnp.where(info_sub == 3 + field, in_lanes, info)
    for number, batch in enumerate(OWN[1:]):
        refs = piece_refs[number * RING : (number + 1) * RING]
        copy_units(fields_ref, batch, refs)
        if INFO_CHUNK in batch:
            for ref in refs:
                ref[batch_tiles(batch) - 1] = info


def join_kernel(batch, *refs):
    out_refs = refs[RING:]
    for distance in range(RING):
        base = 0
        for out_ref, chunk in zip(out_refs, batch):
            out_ref[distance] = refs[distance][base : base + tile_count(chunk)]
            base += tile_count(chunk)
        if INFO_CHUNK in batch:
            out_refs[-1][distance] = refs[distance][batch_tiles(batch) - 1]


def column_kernel(batch, start_ref, weight_ref, *refs):
    sides = [refs[3 * number : 3 * number + 3] for number in range(len(batch))]
    refs = refs[3 * len(batch) :]
    out_refs, rows_refs = refs[:RING], refs[len(refs) - len(batch) :]
    place = lax.axis_index(LAT[2])
    positions = side_places(lax.axis_index(LAT[:2]))
    for chunk, side_refs, rows_ref in zip(batch, sides, rows_refs):
        count = width_of(chunk) * ROWS
        if chunk == INFO_CHUNK:
            for side, ref in zip(positions, side_refs):
                refs[RING][side] = ref[:, count]
        for distance in range(RING):
            band = across(place, distance)
            for side, ref in zip(positions, side_refs):
                rows_ref[pl.ds((side * RING + band) * count, count)] = ref[distance, :count]

    def one_row(row, carry):
        for distance in range(RING):
            first = start_ref[distance, row]
            weights = [weight_ref[step, distance, row] for step in range(4)]
            base = 0
            for chunk, rows_ref in zip(batch, rows_refs):
                width = width_of(chunk)
                total = weights[0] * rows_ref[pl.ds(first * width, width)]
                for step in range(1, 4):
                    total = total + weights[step] * rows_ref[pl.ds((first + step) * width, width)]
                out_refs[distance][pl.ds(base + row * width, width)] = total
                base += ROWS * width
        return carry

    lax.fori_loop(0, ROWS, one_row, 0)


def field_units(field):
    found = []
    for tile in range(QUARTER):
        unit = field * QUARTER + tile
        for number, batch in enumerate(BACK):
            base = 0
            for chunk in batch:
                first, last = CHUNKS[chunk]
                if first <= unit < last:
                    found.append((number, base + unit - first, last - first))
                base += ROWS * (last - first)
    return found


def field_batches(field):
    return sorted({number for number, _, _ in field_units(field)})


def finish_kernel(field, shift_ref, weight_ref, ratio_ref, *refs):
    out_ref, turned_ref = refs[-2], refs[-1]
    batches = field_batches(field)
    place = lax.axis_index(LAT[2])
    owners = [across(place, distance) for distance in range(RING)]
    lane = lax.broadcasted_iota(jnp.int32, (8, LANES), 1)
    scale = ratio_ref[field]

    def ahead(values, step):
        moved = [pltpu.roll(value, LANES - step, 1) for value in values]
        following = moved[1:] + moved[:1]
        return [jnp.where(lane < LANES - step, here, then) for here, then in zip(moved, following)]

    def some_rows(pair, carry):
        for member in range(TOGETHER):
            row = pair * TOGETHER + member
            slot = member * 2 * TILES
            base = shift_ref[row]
            base = jnp.where(base == 0, LON - 1, base - 1)
            whole = base // LANES
            back = LANES - (base - whole * LANES)
            for distance in range(RING):
                for tile, (number, at, width) in enumerate(field_units(field)):
                    piece = refs[batches.index(number) * RING + distance][row * width + at]
                    turned_ref[slot + owners[distance] * QUARTER + tile] = piece
                    turned_ref[slot + TILES + owners[distance] * QUARTER + tile] = piece
            weights = [weight_ref[step, row] * scale for step in range(4)]
            rolled = [pltpu.roll(turned_ref[slot + whole + tile], back, 1) for tile in range(TILES)]
            lined = [jnp.where(lane < back, here, then) for here, then in zip(rolled, rolled[1:] + rolled[:1])]
            next_one = ahead(lined, 1)
            far = ahead([weights[2] * here + weights[3] * then for here, then in zip(lined, next_one)], 2)
            for tile in range(TILES):
                out_ref[row, 0, :, tile * LANES : (tile + 1) * LANES] = (
                    weights[0] * lined[tile] + weights[1] * next_one[tile] + far[tile]
                )
        return carry

    lax.fori_loop(0, ROWS // TOGETHER, some_rows, 0)


def swap(array, axis, partner):
    return lax.ppermute(array, axis, [(i, partner(i)) for i in range(lax.axis_size(axis))])


def exchange(pieces):
    received = {0: pieces[0]}
    for step in PARTNERS:
        received[step] = swap(pieces[step], LAT[2], lambda i, step=step: i ^ step)
    return [received[step] for step in range(RING)]


def both_sides(block):
    groups = lax.axis_size(LAT[:2])
    inner = swap(block, LAT[:2], lambda i: i ^ 1)
    outer = swap(block, LAT[:2], lambda i: (i + 1 if i % 2 else i - 1) % groups)
    return inner, outer


def tiles(*shape):
    return jax.ShapeDtypeStruct((*shape, 8, LANES), jnp.float32)


def per_device(fields, lat_fraction, lon_fraction, lon_shift, departure_row, extents):
    params = pltpu.CompilerParams(vmem_limit_bytes=VMEM_LIMIT)
    pieces = [
        pl.pallas_call(
            pack_first,
            out_shape=[tiles(batch_tiles(OWN[0]))] * RING,
            in_specs=[VMEM],
            out_specs=[VMEM] * RING,
            compiler_params=params,
            name="pack_a",
        )(fields)
    ]
    rest = pl.pallas_call(
        pack_rest,
        out_shape=[tiles(batch_tiles(batch)) for batch in OWN[1:] for _ in range(RING)],
        in_specs=[SMEM] * 4 + [VMEM],
        out_specs=[VMEM] * (RING * (len(OWN) - 1)),
        compiler_params=params,
        name="pack_b",
    )(departure_row, extents, lat_fraction, lon_fraction, fields)
    pieces += [rest[number * RING : (number + 1) * RING] for number in range(len(OWN) - 1)]

    own, inner, outer = {}, {}, {}
    for number, batch in enumerate(OWN):
        received = exchange(pieces[number])
        shapes = [tiles(RING, tile_count(chunk)) for chunk in batch] + [tiles(RING)] * (INFO_CHUNK in batch)
        joined = pl.pallas_call(
            partial(join_kernel, batch),
            out_shape=shapes,
            in_specs=[VMEM] * RING,
            out_specs=[VMEM] * len(shapes),
            compiler_params=params,
            name="join",
        )(*received)
        if INFO_CHUNK in batch:
            ring_info = joined[-1][:, :, :ROWS]
        for chunk, block in zip(batch, joined):
            own[chunk] = block
            inner[chunk], outer[chunk] = both_sides(block)

    ring_start = ring_info[:, 0].astype(jnp.int32)
    ring_weight = jnp.stack(cubic_weights(ring_info[:, 1]))

    gathered = []
    for batch in BACK:
        shapes = [tiles(column_tiles(batch))] * RING + [tiles(3, RING)] * (INFO_CHUNK in batch)
        operands = [part[chunk] for chunk in batch for part in (inner, own, outer)]
        columns = pl.pallas_call(
            partial(column_kernel, batch),
            out_shape=shapes,
            in_specs=[SMEM, SMEM] + [VMEM] * len(operands),
            out_specs=[VMEM] * len(shapes),
            scratch_shapes=[
                pltpu.VMEM((3 * GROUP * width_of(chunk), 8, LANES), jnp.float32) for chunk in batch
            ],
            compiler_params=params,
            name="column",
        )(ring_start, ring_weight, *operands)
        if INFO_CHUNK in batch:
            all_info = columns[RING]
        gathered.append(exchange(columns[:RING]))

    total_rows = lax.axis_size(LAT) * ROWS
    group_row = lax.axis_index(LAT[:2]) * GROUP
    bands = across(lax.axis_index(LAT[2]), jnp.arange(RING, dtype=jnp.int32))
    ring_rows = bands[:, None] * ROWS + jnp.arange(ROWS, dtype=jnp.int32)[None]
    area = jnp.cos(math.pi * ((group_row + ring_rows).astype(jnp.float32) + 0.5) / total_rows - math.pi / 2.0)
    sums = all_info[:, :, 3 : 3 + FIELDS, :ROWS]
    lon_total = sum(cubic_weights(ring_info[:, 2]))
    before = jnp.sum(area[:, None, :] * sums[1], axis=(0, 2))
    after = jnp.zeros((FIELDS,), jnp.float32)
    for side in range(3):
        spots = side * GROUP + ring_rows
        factor = jnp.zeros((RING, ROWS), jnp.float32)
        for step in range(4):
            hit = (ring_start + step)[None, None] == spots[..., None, None]
            share = area * lon_total * ring_weight[step]
            factor = factor + jnp.sum(jnp.where(hit, share[None, None], 0.0), axis=(2, 3))
        after = after + jnp.sum(factor[:, None, :] * sums[side], axis=(0, 2))
    mass = jnp.pad(jnp.concatenate([before, after]), (0, LANES - 2 * FIELDS))
    parties = (LAT[0], LAT[1], "lev")
    spread = jnp.broadcast_to(mass[None, None], (lax.axis_size(parties), 1, LANES))
    spread = lax.all_to_all(spread, parties, 0, 0)
    mass = jnp.sum(spread, axis=(0, 1))
    ratio = mass[:FIELDS] / mass[FIELDS : 2 * FIELDS]
    lon_w = jnp.stack(cubic_weights(lon_fraction))

    result = None
    for field in range(FIELDS):
        operands = [piece for number in field_batches(field) for piece in gathered[number]]
        in_specs = [SMEM, SMEM, SMEM] + [VMEM] * len(operands)
        aliases = {}
        if result is not None:
            operands.append(result)
            in_specs.append(ANY)
            aliases = {len(in_specs) - 1: 0}
        result = pl.pallas_call(
            partial(finish_kernel, field),
            grid=(1,),
            out_shape=jax.ShapeDtypeStruct(fields.shape, jnp.float32),
            in_specs=in_specs,
            out_specs=pl.BlockSpec((ROWS, 1, 8, LON), lambda i, field=field: (0, field, 0, 0)),
            scratch_shapes=[pltpu.VMEM((TOGETHER * 2 * TILES, 8, LANES), jnp.float32)],
            input_output_aliases=aliases,
            compiler_params=params,
            name="finish",
        )(lon_shift, lon_w, ratio, *operands)
    return result


def solution(mesh):
    finer = Mesh(mesh.devices.reshape(4, 8, 4, mesh.shape["lev"]), LAT + ("lev",))
    placed = (P(LAT, None, "lev", None), P(LAT), P(LAT), P(LAT), P(LAT), P(LAT, None))
    return jax.shard_map(
        per_device,
        mesh=finer,
        in_specs=placed,
        out_specs=P(LAT, None, "lev", None),
        check_vma=False,
    )
```

```python
import math
from functools import partial

import jax
import jax.numpy as jnp
from jax import lax
from jax.experimental import pallas as pl
from jax.experimental.pallas import tpu as pltpu
from jax.sharding import Mesh
from jax.sharding import PartitionSpec as P


LAT = ("lat_0", "lat_1", "lat_2")
ROWS = 10
RING = 4
GROUP = RING * ROWS
FIELDS = 3
LANES = 128
QUARTER = 5
TILES = RING * QUARTER
LON = TILES * LANES
CHUNKS = ((0, 3), (3, 9), (9, 13), (13, 15))
PARTNERS = (2, 1, 3)
OWN = ((0,), (1,), (2, 3))
BACK = ((0,), (1,), (2,), (3,))
INFO_CHUNK = 0
TOGETHER = 2
VMEM_LIMIT = 12 * 1024 * 1024


VMEM = pl.BlockSpec(memory_space=pltpu.VMEM)
SMEM = pl.BlockSpec(memory_space=pltpu.SMEM)
ANY = pl.BlockSpec(memory_space=pl.ANY)


def cubic_weights(fraction):
    return (
        -fraction * (fraction - 1.0) * (fraction - 2.0) / 6.0,
        (fraction + 1.0) * (fraction - 1.0) * (fraction - 2.0) / 2.0,
        -(fraction + 1.0) * fraction * (fraction - 2.0) / 2.0,
        (fraction + 1.0) * fraction * (fraction - 1.0) / 6.0,
    )


def across(place, step):
    return jnp.bitwise_xor(place, step)


def side_places(group):
    even = 1 - lax.rem(group, 2)
    return 2 * even, 1, 2 - 2 * even


def width_of(chunk):
    first, last = CHUNKS[chunk]
    return last - first


def tile_count(chunk):
    return ROWS * width_of(chunk) + (1 if chunk == INFO_CHUNK else 0)


def batch_tiles(batch):
    return sum(tile_count(chunk) for chunk in batch)


def column_tiles(batch):
    return sum(ROWS * width_of(chunk) for chunk in batch)


def copy_units(fields_ref, batch, piece_refs):
    place = lax.axis_index(LAT[2])
    for distance in range(RING):
        owner = across(place, distance)
        base = 0
        for chunk in batch:
            first, last = CHUNKS[chunk]
            for unit in range(first, last):
                field, tile = divmod(unit, QUARTER)
                start = pl.multiple_of((owner * QUARTER + tile) * LANES, LANES)
                for row in range(ROWS):
                    piece_refs[distance][base + row * (last - first) + unit - first] = fields_ref[
                        row, field, :, pl.ds(start, LANES)
                    ]
            base += tile_count(chunk)


def pack_first(scalar_ref, fields_ref, *piece_refs):
    first_row = (lax.axis_index(LAT) * ROWS).astype(jnp.float32)
    group_row = (lax.axis_index(LAT[:2]) * GROUP).astype(jnp.float32)
    info_sub = lax.broadcasted_iota(jnp.int32, (8, LANES), 0)
    info_lane = lax.broadcasted_iota(jnp.int32, (8, LANES), 1)
    departure = jnp.zeros((8, LANES), jnp.float32)
    info = jnp.zeros((8, LANES), jnp.float32)
    for row in range(ROWS):
        here = info_lane == row
        departure = jnp.where(here, scalar_ref[row], departure)
        info = jnp.where(here & (info_sub == 1), scalar_ref[ROWS + row], info)
        info = jnp.where(here & (info_sub == 2), scalar_ref[2 * ROWS + row], info)
    low_bound = first_row - scalar_ref[3 * ROWS] * ROWS + 1.0
    high_bound = first_row + (ROWS - 3.0) + scalar_ref[3 * ROWS + 1] * ROWS
    departure = jnp.minimum(jnp.maximum(departure, low_bound), high_bound)
    departure = jnp.minimum(jnp.maximum(departure, 1.0), RING * 32 * ROWS - 3.0)
    info = jnp.where(info_sub == 0, departure - 1.0 - (group_row - GROUP), info)
    sub = lax.broadcasted_iota(jnp.int32, (ROWS, LANES), 0)
    lane = lax.broadcasted_iota(jnp.int32, (ROWS, LANES), 1)
    for field in range(FIELDS):
        total = fields_ref[:, field, :, 0:LANES]
        for tile in range(1, TILES):
            total = total + fields_ref[:, field, :, tile * LANES : (tile + 1) * LANES]
        by_row = jnp.sum(jnp.sum(total, axis=1), axis=1, keepdims=True)
        in_lanes = jnp.sum(jnp.where(sub == lane, by_row, 0.0), axis=0, keepdims=True)
        info = jnp.where(info_sub == 3 + field, in_lanes, info)
    copy_units(fields_ref, OWN[0], piece_refs)
    for ref in piece_refs:
        ref[batch_tiles(OWN[0]) - 1] = info


def pack_rest(fields_ref, *piece_refs):
    for number, batch in enumerate(OWN[1:]):
        copy_units(fields_ref, batch, piece_refs[number * RING : (number + 1) * RING])


def join_kernel(batch, *refs):
    out_refs = refs[RING:]
    for distance in range(RING):
        base = 0
        for out_ref, chunk in zip(out_refs, batch):
            out_ref[distance] = refs[distance][base : base + tile_count(chunk)]
            base += tile_count(chunk)
        if INFO_CHUNK in batch:
            out_refs[-1][distance] = refs[distance][batch_tiles(batch) - 1]


def column_kernel(batch, start_ref, weight_ref, *refs):
    sides = [refs[3 * number : 3 * number + 3] for number in range(len(batch))]
    refs = refs[3 * len(batch) :]
    out_refs, rows_refs = refs[:RING], refs[len(refs) - len(batch) :]
    place = lax.axis_index(LAT[2])
    positions = side_places(lax.axis_index(LAT[:2]))
    for chunk, side_refs, rows_ref in zip(batch, sides, rows_refs):
        count = width_of(chunk) * ROWS
        if chunk == INFO_CHUNK:
            for side, ref in zip(positions, side_refs):
                refs[RING][side] = ref[:, count]
        for distance in range(RING):
            band = across(place, distance)
            for side, ref in zip(positions, side_refs):
                rows_ref[pl.ds((side * RING + band) * count, count)] = ref[distance, :count]

    def one_row(row, carry):
        for distance in range(RING):
            first = start_ref[distance, row]
            weights = [weight_ref[step, distance, row] for step in range(4)]
            base = 0
            for chunk, rows_ref in zip(batch, rows_refs):
                width = width_of(chunk)
                total = weights[0] * rows_ref[pl.ds(first * width, width)]
                for step in range(1, 4):
                    total = total + weights[step] * rows_ref[pl.ds((first + step) * width, width)]
                out_refs[distance][pl.ds(base + row * width, width)] = total
                base += ROWS * width
        return carry

    lax.fori_loop(0, ROWS, one_row, 0)


def field_units(field):
    found = []
    for tile in range(QUARTER):
        unit = field * QUARTER + tile
        for number, batch in enumerate(BACK):
            base = 0
            for chunk in batch:
                first, last = CHUNKS[chunk]
                if first <= unit < last:
                    found.append((number, base + unit - first, last - first))
                base += ROWS * (last - first)
    return found


def field_batches(field):
    return sorted({number for number, _, _ in field_units(field)})


def finish_kernel(field, shift_ref, weight_ref, ratio_ref, *refs):
    out_ref, turned_ref = refs[-2], refs[-1]
    batches = field_batches(field)
    place = lax.axis_index(LAT[2])
    owners = [across(place, distance) for distance in range(RING)]
    lane = lax.broadcasted_iota(jnp.int32, (8, LANES), 1)
    scale = ratio_ref[field]

    def ahead(values, step):
        moved = [pltpu.roll(value, LANES - step, 1) for value in values]
        following = moved[1:] + moved[:1]
        return [jnp.where(lane < LANES - step, here, then) for here, then in zip(moved, following)]

    def some_rows(pair, carry):
        for member in range(TOGETHER):
            row = pair * TOGETHER + member
            slot = member * 2 * TILES
            base = shift_ref[row]
            base = jnp.where(base == 0, LON - 1, base - 1)
            whole = base // LANES
            back = LANES - (base - whole * LANES)
            for distance in range(RING):
                for tile, (number, at, width) in enumerate(field_units(field)):
                    piece = refs[batches.index(number) * RING + distance][row * width + at]
                    turned_ref[slot + owners[distance] * QUARTER + tile] = piece
                    turned_ref[slot + TILES + owners[distance] * QUARTER + tile] = piece
            weights = [weight_ref[step, row] * scale for step in range(4)]
            rolled = [pltpu.roll(turned_ref[slot + whole + tile], back, 1) for tile in range(TILES)]
            lined = [jnp.where(lane < back, here, then) for here, then in zip(rolled, rolled[1:] + rolled[:1])]
            next_one = ahead(lined, 1)
            far = ahead([weights[2] * here + weights[3] * then for here, then in zip(lined, next_one)], 2)
            for tile in range(TILES):
                out_ref[row, 0, :, tile * LANES : (tile + 1) * LANES] = (
                    weights[0] * lined[tile] + weights[1] * next_one[tile] + far[tile]
                )
        return carry

    lax.fori_loop(0, ROWS // TOGETHER, some_rows, 0)


def swap(array, axis, partner):
    return lax.ppermute(array, axis, [(i, partner(i)) for i in range(lax.axis_size(axis))])


def exchange(pieces):
    received = {0: pieces[0]}
    for step in PARTNERS:
        received[step] = swap(pieces[step], LAT[2], lambda i, step=step: i ^ step)
    return [received[step] for step in range(RING)]


def both_sides(block):
    groups = lax.axis_size(LAT[:2])
    inner = swap(block, LAT[:2], lambda i: i ^ 1)
    outer = swap(block, LAT[:2], lambda i: (i + 1 if i % 2 else i - 1) % groups)
    return inner, outer


def tiles(*shape):
    return jax.ShapeDtypeStruct((*shape, 8, LANES), jnp.float32)


def per_device(fields, lat_fraction, lon_fraction, lon_shift, departure_row, extents):
    params = pltpu.CompilerParams(vmem_limit_bytes=VMEM_LIMIT)
    scalars = jnp.concatenate(
        [departure_row.astype(jnp.float32), lat_fraction, lon_fraction, extents[0].astype(jnp.float32)]
    )
    pieces = [
        pl.pallas_call(
            pack_first,
            out_shape=[tiles(batch_tiles(OWN[0]))] * RING,
            in_specs=[SMEM, VMEM],
            out_specs=[VMEM] * RING,
            compiler_params=params,
            name="pack_a",
        )(scalars, fields)
    ]
    rest = pl.pallas_call(
        pack_rest,
        out_shape=[tiles(batch_tiles(batch)) for batch in OWN[1:] for _ in range(RING)],
        in_specs=[VMEM],
        out_specs=[VMEM] * (RING * (len(OWN) - 1)),
        compiler_params=params,
        name="pack_b",
    )(fields)
    pieces += [rest[number * RING : (number + 1) * RING] for number in range(len(OWN) - 1)]

    own, inner, outer = {}, {}, {}
    for number, batch in enumerate(OWN):
        received = exchange(pieces[number])
        shapes = [tiles(RING, tile_count(chunk)) for chunk in batch] + [tiles(RING)] * (INFO_CHUNK in batch)
        joined = pl.pallas_call(
            partial(join_kernel, batch),
            out_shape=shapes,
            in_specs=[VMEM] * RING,
            out_specs=[VMEM] * len(shapes),
            compiler_params=params,
            name="join",
        )(*received)
        if INFO_CHUNK in batch:
            ring_info = joined[-1][:, :, :ROWS]
        for chunk, block in zip(batch, joined):
            own[chunk] = block
            inner[chunk], outer[chunk] = both_sides(block)

    ring_start = ring_info[:, 0].astype(jnp.int32)
    ring_weight = jnp.stack(cubic_weights(ring_info[:, 1]))

    gathered = []
    for batch in BACK:
        shapes = [tiles(column_tiles(batch))] * RING + [tiles(3, RING)] * (INFO_CHUNK in batch)
        operands = [part[chunk] for chunk in batch for part in (inner, own, outer)]
        columns = pl.pallas_call(
            partial(column_kernel, batch),
            out_shape=shapes,
            in_specs=[SMEM, SMEM] + [VMEM] * len(operands),
            out_specs=[VMEM] * len(shapes),
            scratch_shapes=[
                pltpu.VMEM((3 * GROUP * width_of(chunk), 8, LANES), jnp.float32) for chunk in batch
            ],
            compiler_params=params,
            name="column",
        )(ring_start, ring_weight, *operands)
        if INFO_CHUNK in batch:
            all_info = columns[RING]
        gathered.append(exchange(columns[:RING]))

    total_rows = lax.axis_size(LAT) * ROWS
    group_row = lax.axis_index(LAT[:2]) * GROUP
    bands = across(lax.axis_index(LAT[2]), jnp.arange(RING, dtype=jnp.int32))
    ring_rows = bands[:, None] * ROWS + jnp.arange(ROWS, dtype=jnp.int32)[None]
    area = jnp.cos(math.pi * ((group_row + ring_rows).astype(jnp.float32) + 0.5) / total_rows - math.pi / 2.0)
    sums = all_info[:, :, 3 : 3 + FIELDS, :ROWS]
    lon_total = sum(cubic_weights(ring_info[:, 2]))
    before = jnp.sum(area[:, None, :] * sums[1], axis=(0, 2))
    after = jnp.zeros((FIELDS,), jnp.float32)
    for side in range(3):
        spots = side * GROUP + ring_rows
        factor = jnp.zeros((RING, ROWS), jnp.float32)
        for step in range(4):
            hit = (ring_start + step)[None, None] == spots[..., None, None]
            share = area * lon_total * ring_weight[step]
            factor = factor + jnp.sum(jnp.where(hit, share[None, None], 0.0), axis=(2, 3))
        after = after + jnp.sum(factor[:, None, :] * sums[side], axis=(0, 2))
    mass = jnp.pad(jnp.concatenate([before, after]), (0, LANES - 2 * FIELDS))
    parties = (LAT[0], LAT[1], "lev")
    spread = jnp.broadcast_to(mass[None, None], (lax.axis_size(parties), 1, LANES))
    spread = lax.all_to_all(spread, parties, 0, 0)
    mass = jnp.sum(spread, axis=(0, 1))
    ratio = mass[:FIELDS] / mass[FIELDS : 2 * FIELDS]
    lon_w = jnp.stack(cubic_weights(lon_fraction))

    result = None
    for field in range(FIELDS):
        operands = [piece for number in field_batches(field) for piece in gathered[number]]
        in_specs = [SMEM, SMEM, SMEM] + [VMEM] * len(operands)
        aliases = {}
        if result is not None:
            operands.append(result)
            in_specs.append(ANY)
            aliases = {len(in_specs) - 1: 0}
        result = pl.pallas_call(
            partial(finish_kernel, field),
            grid=(1,),
            out_shape=jax.ShapeDtypeStruct(fields.shape, jnp.float32),
            in_specs=in_specs,
            out_specs=pl.BlockSpec((ROWS, 1, 8, LON), lambda i, field=field: (0, field, 0, 0)),
            scratch_shapes=[pltpu.VMEM((TOGETHER * 2 * TILES, 8, LANES), jnp.float32)],
            input_output_aliases=aliases,
            compiler_params=params,
            name="finish",
        )(lon_shift, lon_w, ratio, *operands)
    return result


def solution(mesh):
    finer = Mesh(mesh.devices.reshape(4, 8, 4, mesh.shape["lev"]), LAT + ("lev",))
    placed = (P(LAT, None, "lev", None), P(LAT), P(LAT), P(LAT), P(LAT), P(LAT, None))
    return jax.shard_map(
        per_device,
        mesh=finer,
        in_specs=placed,
        out_specs=P(LAT, None, "lev", None),
        check_vma=False,
    )
```

```python
import math
from functools import partial

import jax
import jax.numpy as jnp
from jax import lax
from jax.experimental import pallas as pl
from jax.experimental.pallas import tpu as pltpu
from jax.sharding import Mesh
from jax.sharding import PartitionSpec as P


LAT = ("lat_0", "lat_1", "lat_2")
ROWS = 10
RING = 4
GROUP = RING * ROWS
FIELDS = 3
LANES = 128
QUARTER = 5
TILES = RING * QUARTER
LON = TILES * LANES
CHUNKS = ((0, 3), (3, 9), (9, 13), (13, 15))
PARTNERS = (2, 1, 3)
OWN = ((0,), (1,), (2, 3))
BACK = ((0,), (1,), (2,), (3,))
INFO_CHUNK = 0
TOGETHER = 5
VMEM_LIMIT = 12 * 1024 * 1024


VMEM = pl.BlockSpec(memory_space=pltpu.VMEM)
SMEM = pl.BlockSpec(memory_space=pltpu.SMEM)
ANY = pl.BlockSpec(memory_space=pl.ANY)


def cubic_weights(fraction):
    return (
        -fraction * (fraction - 1.0) * (fraction - 2.0) / 6.0,
        (fraction + 1.0) * (fraction - 1.0) * (fraction - 2.0) / 2.0,
        -(fraction + 1.0) * fraction * (fraction - 2.0) / 2.0,
        (fraction + 1.0) * fraction * (fraction - 1.0) / 6.0,
    )


def across(place, step):
    return jnp.bitwise_xor(place, step)


def side_places(group):
    even = 1 - lax.rem(group, 2)
    return 2 * even, 1, 2 - 2 * even


def width_of(chunk):
    first, last = CHUNKS[chunk]
    return last - first


def tile_count(chunk):
    return ROWS * width_of(chunk) + (1 if chunk == INFO_CHUNK else 0)


def batch_tiles(batch):
    return sum(tile_count(chunk) for chunk in batch)


def column_tiles(batch):
    return sum(ROWS * width_of(chunk) for chunk in batch)


def copy_units(fields_ref, batch, piece_refs):
    place = lax.axis_index(LAT[2])
    for distance in range(RING):
        owner = across(place, distance)
        base = 0
        for chunk in batch:
            first, last = CHUNKS[chunk]
            for unit in range(first, last):
                field, tile = divmod(unit, QUARTER)
                start = pl.multiple_of((owner * QUARTER + tile) * LANES, LANES)
                for row in range(ROWS):
                    piece_refs[distance][base + row * (last - first) + unit - first] = fields_ref[
                        row, field, :, pl.ds(start, LANES)
                    ]
            base += tile_count(chunk)


def pack_first(extents_ref, scalar_ref, fields_ref, *piece_refs):
    first_row = (lax.axis_index(LAT) * ROWS).astype(jnp.float32)
    group_row = (lax.axis_index(LAT[:2]) * GROUP).astype(jnp.float32)
    info_sub = lax.broadcasted_iota(jnp.int32, (8, LANES), 0)
    info_lane = lax.broadcasted_iota(jnp.int32, (8, LANES), 1)
    departure = jnp.zeros((8, LANES), jnp.float32)
    info = jnp.zeros((8, LANES), jnp.float32)
    for row in range(ROWS):
        here = info_lane == row
        departure = jnp.where(here, scalar_ref[row], departure)
        info = jnp.where(here & (info_sub == 1), scalar_ref[ROWS + row], info)
        info = jnp.where(here & (info_sub == 2), scalar_ref[2 * ROWS + row], info)
    low_bound = first_row - (extents_ref[0, 0] * ROWS).astype(jnp.float32) + 1.0
    high_bound = first_row + (extents_ref[0, 1] * ROWS).astype(jnp.float32) + (ROWS - 3.0)
    departure = jnp.minimum(jnp.maximum(departure, low_bound), high_bound)
    departure = jnp.minimum(jnp.maximum(departure, 1.0), RING * 32 * ROWS - 3.0)
    info = jnp.where(info_sub == 0, departure - 1.0 - (group_row - GROUP), info)
    sub = lax.broadcasted_iota(jnp.int32, (ROWS, LANES), 0)
    lane = lax.broadcasted_iota(jnp.int32, (ROWS, LANES), 1)
    for field in range(FIELDS):
        total = fields_ref[:, field, :, 0:LANES]
        for tile in range(1, TILES):
            total = total + fields_ref[:, field, :, tile * LANES : (tile + 1) * LANES]
        by_row = jnp.sum(jnp.sum(total, axis=1), axis=1, keepdims=True)
        in_lanes = jnp.sum(jnp.where(sub == lane, by_row, 0.0), axis=0, keepdims=True)
        info = jnp.where(info_sub == 3 + field, in_lanes, info)
    copy_units(fields_ref, OWN[0], piece_refs)
    for ref in piece_refs:
        ref[batch_tiles(OWN[0]) - 1] = info


def pack_rest(fields_ref, *piece_refs):
    for number, batch in enumerate(OWN[1:]):
        copy_units(fields_ref, batch, piece_refs[number * RING : (number + 1) * RING])


def join_kernel(batch, *refs):
    out_refs = refs[RING:]
    for distance in range(RING):
        base = 0
        for out_ref, chunk in zip(out_refs, batch):
            out_ref[distance] = refs[distance][base : base + tile_count(chunk)]
            base += tile_count(chunk)
        if INFO_CHUNK in batch:
            out_refs[-1][distance] = refs[distance][batch_tiles(batch) - 1]


def column_kernel(batch, start_ref, weight_ref, *refs):
    sides = [refs[3 * number : 3 * number + 3] for number in range(len(batch))]
    refs = refs[3 * len(batch) :]
    out_refs, rows_refs = refs[:RING], refs[len(refs) - len(batch) :]
    place = lax.axis_index(LAT[2])
    positions = side_places(lax.axis_index(LAT[:2]))
    for chunk, side_refs, rows_ref in zip(batch, sides, rows_refs):
        count = width_of(chunk) * ROWS
        if chunk == INFO_CHUNK:
            for side, ref in zip(positions, side_refs):
                refs[RING][side] = ref[:, count]
        for distance in range(RING):
            band = across(place, distance)
            for side, ref in zip(positions, side_refs):
                rows_ref[pl.ds((side * RING + band) * count, count)] = ref[distance, :count]

    def one_row(row, carry):
        for distance in range(RING):
            first = start_ref[distance, row]
            weights = [weight_ref[step, distance, row] for step in range(4)]
            base = 0
            for chunk, rows_ref in zip(batch, rows_refs):
                width = width_of(chunk)
                total = weights[0] * rows_ref[pl.ds(first * width, width)]
                for step in range(1, 4):
                    total = total + weights[step] * rows_ref[pl.ds((first + step) * width, width)]
                out_refs[distance][pl.ds(base + row * width, width)] = total
                base += ROWS * width
        return carry

    lax.fori_loop(0, ROWS, one_row, 0)


def field_units(field):
    found = []
    for tile in range(QUARTER):
        unit = field * QUARTER + tile
        for number, batch in enumerate(BACK):
            base = 0
            for chunk in batch:
                first, last = CHUNKS[chunk]
                if first <= unit < last:
                    found.append((number, base + unit - first, last - first))
                base += ROWS * (last - first)
    return found


def field_batches(field):
    return sorted({number for number, _, _ in field_units(field)})


def finish_kernel(field, shift_ref, weight_ref, ratio_ref, *refs):
    out_ref, turned_ref = refs[-2], refs[-1]
    batches = field_batches(field)
    place = lax.axis_index(LAT[2])
    owners = [across(place, distance) for distance in range(RING)]
    lane = lax.broadcasted_iota(jnp.int32, (8, LANES), 1)
    scale = ratio_ref[field]

    def ahead(values, step):
        moved = [pltpu.roll(value, LANES - step, 1) for value in values]
        following = moved[1:] + moved[:1]
        return [jnp.where(lane < LANES - step, here, then) for here, then in zip(moved, following)]

    def some_rows(pair, carry):
        for member in range(TOGETHER):
            row = pair * TOGETHER + member
            slot = member * 2 * TILES
            base = shift_ref[row]
            base = jnp.where(base == 0, LON - 1, base - 1)
            whole = base // LANES
            back = LANES - (base - whole * LANES)
            for distance in range(RING):
                for tile, (number, at, width) in enumerate(field_units(field)):
                    piece = refs[batches.index(number) * RING + distance][row * width + at]
                    turned_ref[slot + owners[distance] * QUARTER + tile] = piece
                    turned_ref[slot + TILES + owners[distance] * QUARTER + tile] = piece
            weights = [weight_ref[step, row] * scale for step in range(4)]
            rolled = [pltpu.roll(turned_ref[slot + whole + tile], back, 1) for tile in range(TILES)]
            lined = [jnp.where(lane < back, here, then) for here, then in zip(rolled, rolled[1:] + rolled[:1])]
            next_one = ahead(lined, 1)
            far = ahead([weights[2] * here + weights[3] * then for here, then in zip(lined, next_one)], 2)
            for tile in range(TILES):
                out_ref[row, 0, :, tile * LANES : (tile + 1) * LANES] = (
                    weights[0] * lined[tile] + weights[1] * next_one[tile] + far[tile]
                )
        return carry

    lax.fori_loop(0, ROWS // TOGETHER, some_rows, 0)


def swap(array, axis, partner):
    return lax.ppermute(array, axis, [(i, partner(i)) for i in range(lax.axis_size(axis))])


def exchange(pieces):
    received = {0: pieces[0]}
    for step in PARTNERS:
        received[step] = swap(pieces[step], LAT[2], lambda i, step=step: i ^ step)
    return [received[step] for step in range(RING)]


def both_sides(block):
    groups = lax.axis_size(LAT[:2])
    inner = swap(block, LAT[:2], lambda i: i ^ 1)
    outer = swap(block, LAT[:2], lambda i: (i + 1 if i % 2 else i - 1) % groups)
    return inner, outer


def tiles(*shape):
    return jax.ShapeDtypeStruct((*shape, 8, LANES), jnp.float32)


def per_device(fields, lat_fraction, lon_fraction, lon_shift, departure_row, extents):
    params = pltpu.CompilerParams(vmem_limit_bytes=VMEM_LIMIT)
    scalars = jnp.concatenate([departure_row.astype(jnp.float32), lat_fraction, lon_fraction])
    pieces = [
        pl.pallas_call(
            pack_first,
            out_shape=[tiles(batch_tiles(OWN[0]))] * RING,
            in_specs=[SMEM, SMEM, VMEM],
            out_specs=[VMEM] * RING,
            compiler_params=params,
            name="pack_a",
        )(extents, scalars, fields)
    ]
    rest = pl.pallas_call(
        pack_rest,
        out_shape=[tiles(batch_tiles(batch)) for batch in OWN[1:] for _ in range(RING)],
        in_specs=[VMEM],
        out_specs=[VMEM] * (RING * (len(OWN) - 1)),
        compiler_params=params,
        name="pack_b",
    )(fields)
    pieces += [rest[number * RING : (number + 1) * RING] for number in range(len(OWN) - 1)]

    own, inner, outer = {}, {}, {}
    for number, batch in enumerate(OWN):
        received = exchange(pieces[number])
        shapes = [tiles(RING, tile_count(chunk)) for chunk in batch] + [tiles(RING)] * (INFO_CHUNK in batch)
        joined = pl.pallas_call(
            partial(join_kernel, batch),
            out_shape=shapes,
            in_specs=[VMEM] * RING,
            out_specs=[VMEM] * len(shapes),
            compiler_params=params,
            name="join",
        )(*received)
        if INFO_CHUNK in batch:
            ring_info = joined[-1][:, :, :ROWS]
        for chunk, block in zip(batch, joined):
            own[chunk] = block
            inner[chunk], outer[chunk] = both_sides(block)

    ring_start = ring_info[:, 0].astype(jnp.int32)
    ring_weight = jnp.stack(cubic_weights(ring_info[:, 1]))

    gathered = []
    for batch in BACK:
        shapes = [tiles(column_tiles(batch))] * RING + [tiles(3, RING)] * (INFO_CHUNK in batch)
        operands = [part[chunk] for chunk in batch for part in (inner, own, outer)]
        columns = pl.pallas_call(
            partial(column_kernel, batch),
            out_shape=shapes,
            in_specs=[SMEM, SMEM] + [VMEM] * len(operands),
            out_specs=[VMEM] * len(shapes),
            scratch_shapes=[
                pltpu.VMEM((3 * GROUP * width_of(chunk), 8, LANES), jnp.float32) for chunk in batch
            ],
            compiler_params=params,
            name="column",
        )(ring_start, ring_weight, *operands)
        if INFO_CHUNK in batch:
            all_info = columns[RING]
        gathered.append(exchange(columns[:RING]))

    total_rows = lax.axis_size(LAT) * ROWS
    group_row = lax.axis_index(LAT[:2]) * GROUP
    bands = across(lax.axis_index(LAT[2]), jnp.arange(RING, dtype=jnp.int32))
    ring_rows = bands[:, None] * ROWS + jnp.arange(ROWS, dtype=jnp.int32)[None]
    area = jnp.cos(math.pi * ((group_row + ring_rows).astype(jnp.float32) + 0.5) / total_rows - math.pi / 2.0)
    sums = all_info[:, :, 3 : 3 + FIELDS, :ROWS]
    lon_total = sum(cubic_weights(ring_info[:, 2]))
    before = jnp.sum(area[:, None, :] * sums[1], axis=(0, 2))
    after = jnp.zeros((FIELDS,), jnp.float32)
    for side in range(3):
        spots = side * GROUP + ring_rows
        factor = jnp.zeros((RING, ROWS), jnp.float32)
        for step in range(4):
            hit = (ring_start + step)[None, None] == spots[..., None, None]
            share = area * lon_total * ring_weight[step]
            factor = factor + jnp.sum(jnp.where(hit, share[None, None], 0.0), axis=(2, 3))
        after = after + jnp.sum(factor[:, None, :] * sums[side], axis=(0, 2))
    mass = jnp.pad(jnp.concatenate([before, after]), (0, LANES - 2 * FIELDS))
    parties = (LAT[0], LAT[1], "lev")
    spread = jnp.broadcast_to(mass[None, None], (lax.axis_size(parties), 1, LANES))
    spread = lax.all_to_all(spread, parties, 0, 0)
    mass = jnp.sum(spread, axis=(0, 1))
    ratio = mass[:FIELDS] / mass[FIELDS : 2 * FIELDS]
    lon_w = jnp.stack(cubic_weights(lon_fraction))

    result = None
    for field in range(FIELDS):
        operands = [piece for number in field_batches(field) for piece in gathered[number]]
        in_specs = [SMEM, SMEM, SMEM] + [VMEM] * len(operands)
        aliases = {}
        if result is not None:
            operands.append(result)
            in_specs.append(ANY)
            aliases = {len(in_specs) - 1: 0}
        result = pl.pallas_call(
            partial(finish_kernel, field),
            grid=(1,),
            out_shape=jax.ShapeDtypeStruct(fields.shape, jnp.float32),
            in_specs=in_specs,
            out_specs=pl.BlockSpec((ROWS, 1, 8, LON), lambda i, field=field: (0, field, 0, 0)),
            scratch_shapes=[pltpu.VMEM((TOGETHER * 2 * TILES, 8, LANES), jnp.float32)],
            input_output_aliases=aliases,
            compiler_params=params,
            name="finish",
        )(lon_shift, lon_w, ratio, *operands)
    return result


def solution(mesh):
    finer = Mesh(mesh.devices.reshape(4, 8, 4, mesh.shape["lev"]), LAT + ("lev",))
    placed = (P(LAT, None, "lev", None), P(LAT), P(LAT), P(LAT), P(LAT), P(LAT, None))
    return jax.shard_map(
        per_device,
        mesh=finer,
        in_specs=placed,
        out_specs=P(LAT, None, "lev", None),
        check_vma=False,
    )
```

```python
import math
from functools import partial

import jax
import jax.numpy as jnp
from jax import lax
from jax.experimental import pallas as pl
from jax.experimental.pallas import tpu as pltpu
from jax.sharding import Mesh
from jax.sharding import PartitionSpec as P


LAT = ("lat_0", "lat_1", "lat_2")
ROWS = 10
RING = 4
GROUP = RING * ROWS
FIELDS = 3
LANES = 128
QUARTER = 5
TILES = RING * QUARTER
LON = TILES * LANES
CHUNKS = ((0, 4), (4, 11), (11, 15))
PARTNERS = (2, 1, 3)
OWN = ((0,), (1,), (2,))
BACK = ((0,), (1,), (2,))
INFO_CHUNK = 0
TOGETHER = 5
VMEM_LIMIT = 12 * 1024 * 1024


VMEM = pl.BlockSpec(memory_space=pltpu.VMEM)
SMEM = pl.BlockSpec(memory_space=pltpu.SMEM)
ANY = pl.BlockSpec(memory_space=pl.ANY)


def cubic_weights(fraction):
    return (
        -fraction * (fraction - 1.0) * (fraction - 2.0) / 6.0,
        (fraction + 1.0) * (fraction - 1.0) * (fraction - 2.0) / 2.0,
        -(fraction + 1.0) * fraction * (fraction - 2.0) / 2.0,
        (fraction + 1.0) * fraction * (fraction - 1.0) / 6.0,
    )


def across(place, step):
    return jnp.bitwise_xor(place, step)


def side_places(group):
    even = 1 - lax.rem(group, 2)
    return 2 * even, 1, 2 - 2 * even


def width_of(chunk):
    first, last = CHUNKS[chunk]
    return last - first


def tile_count(chunk):
    return ROWS * width_of(chunk) + (1 if chunk == INFO_CHUNK else 0)


def batch_tiles(batch):
    return sum(tile_count(chunk) for chunk in batch)


def column_tiles(batch):
    return sum(ROWS * width_of(chunk) for chunk in batch)


def copy_units(fields_ref, batch, piece_refs):
    place = lax.axis_index(LAT[2])
    for distance in range(RING):
        owner = across(place, distance)
        base = 0
        for chunk in batch:
            first, last = CHUNKS[chunk]
            for unit in range(first, last):
                field, tile = divmod(unit, QUARTER)
                start = pl.multiple_of((owner * QUARTER + tile) * LANES, LANES)
                for row in range(ROWS):
                    piece_refs[distance][base + row * (last - first) + unit - first] = fields_ref[
                        row, field, :, pl.ds(start, LANES)
                    ]
            base += tile_count(chunk)


def pack_first(extents_ref, scalar_ref, fields_ref, *piece_refs):
    first_row = (lax.axis_index(LAT) * ROWS).astype(jnp.float32)
    group_row = (lax.axis_index(LAT[:2]) * GROUP).astype(jnp.float32)
    info_sub = lax.broadcasted_iota(jnp.int32, (8, LANES), 0)
    info_lane = lax.broadcasted_iota(jnp.int32, (8, LANES), 1)
    departure = jnp.zeros((8, LANES), jnp.float32)
    info = jnp.zeros((8, LANES), jnp.float32)
    for row in range(ROWS):
        here = info_lane == row
        departure = jnp.where(here, scalar_ref[row], departure)
        info = jnp.where(here & (info_sub == 1), scalar_ref[ROWS + row], info)
        info = jnp.where(here & (info_sub == 2), scalar_ref[2 * ROWS + row], info)
    low_bound = first_row - (extents_ref[0, 0] * ROWS).astype(jnp.float32) + 1.0
    high_bound = first_row + (extents_ref[0, 1] * ROWS).astype(jnp.float32) + (ROWS - 3.0)
    departure = jnp.minimum(jnp.maximum(departure, low_bound), high_bound)
    departure = jnp.minimum(jnp.maximum(departure, 1.0), RING * 32 * ROWS - 3.0)
    info = jnp.where(info_sub == 0, departure - 1.0 - (group_row - GROUP), info)
    sub = lax.broadcasted_iota(jnp.int32, (ROWS, LANES), 0)
    lane = lax.broadcasted_iota(jnp.int32, (ROWS, LANES), 1)
    for field in range(FIELDS):
        total = fields_ref[:, field, :, 0:LANES]
        for tile in range(1, TILES):
            total = total + fields_ref[:, field, :, tile * LANES : (tile + 1) * LANES]
        by_row = jnp.sum(jnp.sum(total, axis=1), axis=1, keepdims=True)
        in_lanes = jnp.sum(jnp.where(sub == lane, by_row, 0.0), axis=0, keepdims=True)
        info = jnp.where(info_sub == 3 + field, in_lanes, info)
    copy_units(fields_ref, OWN[0], piece_refs)
    for ref in piece_refs:
        ref[batch_tiles(OWN[0]) - 1] = info


def pack_rest(fields_ref, *piece_refs):
    for number, batch in enumerate(OWN[1:]):
        copy_units(fields_ref, batch, piece_refs[number * RING : (number + 1) * RING])


def join_kernel(batch, *refs):
    out_refs = refs[RING:]
    for distance in range(RING):
        base = 0
        for out_ref, chunk in zip(out_refs, batch):
            out_ref[distance] = refs[distance][base : base + tile_count(chunk)]
            base += tile_count(chunk)
        if INFO_CHUNK in batch:
            out_refs[-1][distance] = refs[distance][batch_tiles(batch) - 1]


def column_kernel(batch, start_ref, weight_ref, *refs):
    sides = [refs[3 * number : 3 * number + 3] for number in range(len(batch))]
    refs = refs[3 * len(batch) :]
    out_refs, rows_refs = refs[:RING], refs[len(refs) - len(batch) :]
    place = lax.axis_index(LAT[2])
    positions = side_places(lax.axis_index(LAT[:2]))
    for chunk, side_refs, rows_ref in zip(batch, sides, rows_refs):
        count = width_of(chunk) * ROWS
        if chunk == INFO_CHUNK:
            for side, ref in zip(positions, side_refs):
                refs[RING][side] = ref[:, count]
        for distance in range(RING):
            band = across(place, distance)
            for side, ref in zip(positions, side_refs):
                rows_ref[pl.ds((side * RING + band) * count, count)] = ref[distance, :count]

    def one_row(row, carry):
        for distance in range(RING):
            first = start_ref[distance, row]
            weights = [weight_ref[step, distance, row] for step in range(4)]
            base = 0
            for chunk, rows_ref in zip(batch, rows_refs):
                width = width_of(chunk)
                total = weights[0] * rows_ref[pl.ds(first * width, width)]
                for step in range(1, 4):
                    total = total + weights[step] * rows_ref[pl.ds((first + step) * width, width)]
                out_refs[distance][pl.ds(base + row * width, width)] = total
                base += ROWS * width
        return carry

    lax.fori_loop(0, ROWS, one_row, 0)


def field_units(field):
    found = []
    for tile in range(QUARTER):
        unit = field * QUARTER + tile
        for number, batch in enumerate(BACK):
            base = 0
            for chunk in batch:
                first, last = CHUNKS[chunk]
                if first <= unit < last:
                    found.append((number, base + unit - first, last - first))
                base += ROWS * (last - first)
    return found


def field_batches(field):
    return sorted({number for number, _, _ in field_units(field)})


def finish_kernel(field, shift_ref, weight_ref, ratio_ref, *refs):
    out_ref, turned_ref = refs[-2], refs[-1]
    batches = field_batches(field)
    place = lax.axis_index(LAT[2])
    owners = [across(place, distance) for distance in range(RING)]
    lane = lax.broadcasted_iota(jnp.int32, (8, LANES), 1)
    scale = ratio_ref[field]

    def ahead(values, step):
        moved = [pltpu.roll(value, LANES - step, 1) for value in values]
        following = moved[1:] + moved[:1]
        return [jnp.where(lane < LANES - step, here, then) for here, then in zip(moved, following)]

    def some_rows(pair, carry):
        for member in range(TOGETHER):
            row = pair * TOGETHER + member
            slot = member * 2 * TILES
            base = shift_ref[row]
            base = jnp.where(base == 0, LON - 1, base - 1)
            whole = base // LANES
            back = LANES - (base - whole * LANES)
            for distance in range(RING):
                for tile, (number, at, width) in enumerate(field_units(field)):
                    piece = refs[batches.index(number) * RING + distance][row * width + at]
                    turned_ref[slot + owners[distance] * QUARTER + tile] = piece
                    turned_ref[slot + TILES + owners[distance] * QUARTER + tile] = piece
            weights = [weight_ref[step, row] * scale for step in range(4)]
            rolled = [pltpu.roll(turned_ref[slot + whole + tile], back, 1) for tile in range(TILES)]
            lined = [jnp.where(lane < back, here, then) for here, then in zip(rolled, rolled[1:] + rolled[:1])]
            next_one = ahead(lined, 1)
            far = ahead([weights[2] * here + weights[3] * then for here, then in zip(lined, next_one)], 2)
            for tile in range(TILES):
                out_ref[row, 0, :, tile * LANES : (tile + 1) * LANES] = (
                    weights[0] * lined[tile] + weights[1] * next_one[tile] + far[tile]
                )
        return carry

    lax.fori_loop(0, ROWS // TOGETHER, some_rows, 0)


def swap(array, axis, partner):
    return lax.ppermute(array, axis, [(i, partner(i)) for i in range(lax.axis_size(axis))])


def exchange(pieces):
    received = {0: pieces[0]}
    for step in PARTNERS:
        received[step] = swap(pieces[step], LAT[2], lambda i, step=step: i ^ step)
    return [received[step] for step in range(RING)]


def both_sides(block):
    groups = lax.axis_size(LAT[:2])
    inner = swap(block, LAT[:2], lambda i: i ^ 1)
    outer = swap(block, LAT[:2], lambda i: (i + 1 if i % 2 else i - 1) % groups)
    return inner, outer


def tiles(*shape):
    return jax.ShapeDtypeStruct((*shape, 8, LANES), jnp.float32)


def per_device(fields, lat_fraction, lon_fraction, lon_shift, departure_row, extents):
    params = pltpu.CompilerParams(vmem_limit_bytes=VMEM_LIMIT)
    scalars = jnp.concatenate([departure_row.astype(jnp.float32), lat_fraction, lon_fraction])
    pieces = [
        pl.pallas_call(
            pack_first,
            out_shape=[tiles(batch_tiles(OWN[0]))] * RING,
            in_specs=[SMEM, SMEM, VMEM],
            out_specs=[VMEM] * RING,
            compiler_params=params,
            name="pack_a",
        )(extents, scalars, fields)
    ]
    rest = pl.pallas_call(
        pack_rest,
        out_shape=[tiles(batch_tiles(batch)) for batch in OWN[1:] for _ in range(RING)],
        in_specs=[VMEM],
        out_specs=[VMEM] * (RING * (len(OWN) - 1)),
        compiler_params=params,
        name="pack_b",
    )(fields)
    pieces += [rest[number * RING : (number + 1) * RING] for number in range(len(OWN) - 1)]

    own, inner, outer = {}, {}, {}
    for number, batch in enumerate(OWN):
        received = exchange(pieces[number])
        shapes = [tiles(RING, tile_count(chunk)) for chunk in batch] + [tiles(RING)] * (INFO_CHUNK in batch)
        joined = pl.pallas_call(
            partial(join_kernel, batch),
            out_shape=shapes,
            in_specs=[VMEM] * RING,
            out_specs=[VMEM] * len(shapes),
            compiler_params=params,
            name="join",
        )(*received)
        if INFO_CHUNK in batch:
            ring_info = joined[-1][:, :, :ROWS]
        for chunk, block in zip(batch, joined):
            own[chunk] = block
            inner[chunk], outer[chunk] = both_sides(block)

    ring_start = ring_info[:, 0].astype(jnp.int32)
    ring_weight = jnp.stack(cubic_weights(ring_info[:, 1]))

    gathered = []
    for batch in BACK:
        shapes = [tiles(column_tiles(batch))] * RING + [tiles(3, RING)] * (INFO_CHUNK in batch)
        operands = [part[chunk] for chunk in batch for part in (inner, own, outer)]
        columns = pl.pallas_call(
            partial(column_kernel, batch),
            out_shape=shapes,
            in_specs=[SMEM, SMEM] + [VMEM] * len(operands),
            out_specs=[VMEM] * len(shapes),
            scratch_shapes=[
                pltpu.VMEM((3 * GROUP * width_of(chunk), 8, LANES), jnp.float32) for chunk in batch
            ],
            compiler_params=params,
            name="column",
        )(ring_start, ring_weight, *operands)
        if INFO_CHUNK in batch:
            all_info = columns[RING]
        gathered.append(exchange(columns[:RING]))

    total_rows = lax.axis_size(LAT) * ROWS
    group_row = lax.axis_index(LAT[:2]) * GROUP
    bands = across(lax.axis_index(LAT[2]), jnp.arange(RING, dtype=jnp.int32))
    ring_rows = bands[:, None] * ROWS + jnp.arange(ROWS, dtype=jnp.int32)[None]
    area = jnp.cos(math.pi * ((group_row + ring_rows).astype(jnp.float32) + 0.5) / total_rows - math.pi / 2.0)
    sums = all_info[:, :, 3 : 3 + FIELDS, :ROWS]
    lon_total = sum(cubic_weights(ring_info[:, 2]))
    before = jnp.sum(area[:, None, :] * sums[1], axis=(0, 2))
    after = jnp.zeros((FIELDS,), jnp.float32)
    for side in range(3):
        spots = side * GROUP + ring_rows
        factor = jnp.zeros((RING, ROWS), jnp.float32)
        for step in range(4):
            hit = (ring_start + step)[None, None] == spots[..., None, None]
            share = area * lon_total * ring_weight[step]
            factor = factor + jnp.sum(jnp.where(hit, share[None, None], 0.0), axis=(2, 3))
        after = after + jnp.sum(factor[:, None, :] * sums[side], axis=(0, 2))
    mass = jnp.pad(jnp.concatenate([before, after]), (0, LANES - 2 * FIELDS))
    parties = (LAT[0], LAT[1], "lev")
    spread = jnp.broadcast_to(mass[None, None], (lax.axis_size(parties), 1, LANES))
    spread = lax.all_to_all(spread, parties, 0, 0)
    mass = jnp.sum(spread, axis=(0, 1))
    ratio = mass[:FIELDS] / mass[FIELDS : 2 * FIELDS]
    lon_w = jnp.stack(cubic_weights(lon_fraction))

    result = None
    for field in range(FIELDS):
        operands = [piece for number in field_batches(field) for piece in gathered[number]]
        in_specs = [SMEM, SMEM, SMEM] + [VMEM] * len(operands)
        aliases = {}
        if result is not None:
            operands.append(result)
            in_specs.append(ANY)
            aliases = {len(in_specs) - 1: 0}
        result = pl.pallas_call(
            partial(finish_kernel, field),
            grid=(1,),
            out_shape=jax.ShapeDtypeStruct(fields.shape, jnp.float32),
            in_specs=in_specs,
            out_specs=pl.BlockSpec((ROWS, 1, 8, LON), lambda i, field=field: (0, field, 0, 0)),
            scratch_shapes=[pltpu.VMEM((TOGETHER * 2 * TILES, 8, LANES), jnp.float32)],
            input_output_aliases=aliases,
            compiler_params=params,
            name="finish",
        )(lon_shift, lon_w, ratio, *operands)
    return result


def solution(mesh):
    finer = Mesh(mesh.devices.reshape(4, 8, 4, mesh.shape["lev"]), LAT + ("lev",))
    placed = (P(LAT, None, "lev", None), P(LAT), P(LAT), P(LAT), P(LAT), P(LAT, None))
    return jax.shard_map(
        per_device,
        mesh=finer,
        in_specs=placed,
        out_specs=P(LAT, None, "lev", None),
        check_vma=False,
    )
```

```python
import math
from functools import partial

import jax
import jax.numpy as jnp
from jax import lax
from jax.experimental import pallas as pl
from jax.experimental.pallas import tpu as pltpu
from jax.sharding import Mesh
from jax.sharding import PartitionSpec as P


LAT = ("lat_0", "lat_1", "lat_2")
ROWS = 10
RING = 4
GROUP = RING * ROWS
FIELDS = 3
LANES = 128
QUARTER = 5
TILES = RING * QUARTER
LON = TILES * LANES
CHUNKS = ((0, 4), (4, 11), (11, 15))
PARTNERS = (2, 1, 3)
OWN = ((0,), (1,), (2,))
BACK = ((0,), (1,), (2,))
SUMS_CHUNK = 0
INFO_CHUNK = 1
MARKED = (SUMS_CHUNK, INFO_CHUNK)
TOGETHER = 5
VMEM_LIMIT = 12 * 1024 * 1024


VMEM = pl.BlockSpec(memory_space=pltpu.VMEM)
SMEM = pl.BlockSpec(memory_space=pltpu.SMEM)
ANY = pl.BlockSpec(memory_space=pl.ANY)


def cubic_weights(fraction):
    return (
        -fraction * (fraction - 1.0) * (fraction - 2.0) / 6.0,
        (fraction + 1.0) * (fraction - 1.0) * (fraction - 2.0) / 2.0,
        -(fraction + 1.0) * fraction * (fraction - 2.0) / 2.0,
        (fraction + 1.0) * fraction * (fraction - 1.0) / 6.0,
    )


def across(place, step):
    return jnp.bitwise_xor(place, step)


def side_places(group):
    even = 1 - lax.rem(group, 2)
    return 2 * even, 1, 2 - 2 * even


def width_of(chunk):
    first, last = CHUNKS[chunk]
    return last - first


def tile_count(chunk):
    return ROWS * width_of(chunk) + (1 if chunk in MARKED else 0)


def batch_tiles(batch):
    return sum(tile_count(chunk) for chunk in batch)


def column_tiles(batch):
    return sum(ROWS * width_of(chunk) for chunk in batch)


def copy_units(fields_ref, batch, piece_refs):
    place = lax.axis_index(LAT[2])
    for distance in range(RING):
        owner = across(place, distance)
        base = 0
        for chunk in batch:
            first, last = CHUNKS[chunk]
            for unit in range(first, last):
                field, tile = divmod(unit, QUARTER)
                start = pl.multiple_of((owner * QUARTER + tile) * LANES, LANES)
                for row in range(ROWS):
                    piece_refs[distance][base + row * (last - first) + unit - first] = fields_ref[
                        row, field, :, pl.ds(start, LANES)
                    ]
            base += tile_count(chunk)


def pack_first(fields_ref, *piece_refs):
    sub = lax.broadcasted_iota(jnp.int32, (ROWS, LANES), 0)
    lane = lax.broadcasted_iota(jnp.int32, (ROWS, LANES), 1)
    sums_sub = lax.broadcasted_iota(jnp.int32, (8, LANES), 0)
    sums = jnp.zeros((8, LANES), jnp.float32)
    for field in range(FIELDS):
        total = fields_ref[:, field, :, 0:LANES]
        for tile in range(1, TILES):
            total = total + fields_ref[:, field, :, tile * LANES : (tile + 1) * LANES]
        by_row = jnp.sum(jnp.sum(total, axis=1), axis=1, keepdims=True)
        in_lanes = jnp.sum(jnp.where(sub == lane, by_row, 0.0), axis=0, keepdims=True)
        sums = jnp.where(sums_sub == field, in_lanes, sums)
    copy_units(fields_ref, OWN[0], piece_refs)
    for ref in piece_refs:
        ref[batch_tiles(OWN[0]) - 1] = sums


def pack_second(departure_ref, extents_ref, lat_ref, lon_ref, fields_ref, *piece_refs):
    first_row = lax.axis_index(LAT) * ROWS
    group_row = lax.axis_index(LAT[:2]) * GROUP
    low_bound = first_row - extents_ref[0, 0] * ROWS + 1
    high_bound = first_row + ROWS - 3 + extents_ref[0, 1] * ROWS
    info_sub = lax.broadcasted_iota(jnp.int32, (8, LANES), 0)
    info_lane = lax.broadcasted_iota(jnp.int32, (8, LANES), 1)
    starts = jnp.zeros((8, LANES), jnp.int32)
    info = jnp.zeros((8, LANES), jnp.float32)
    for row in range(ROWS):
        departure = jnp.clip(departure_ref[row], low_bound, high_bound)
        departure = jnp.clip(departure, 1, RING * 32 * ROWS - 3)
        here = info_lane == row
        starts = jnp.where(here, departure - 1 - (group_row - GROUP), starts)
        info = jnp.where(here & (info_sub == 1), lat_ref[row], info)
        info = jnp.where(here & (info_sub == 2), lon_ref[row], info)
    info = jnp.where(info_sub == 0, starts.astype(jnp.float32), info)
    copy_units(fields_ref, OWN[1], piece_refs)
    for ref in piece_refs:
        ref[batch_tiles(OWN[1]) - 1] = info


def pack_third(fields_ref, *piece_refs):
    copy_units(fields_ref, OWN[2], piece_refs)


def join_kernel(batch, *refs):
    out_refs = refs[RING:]
    for distance in range(RING):
        base = 0
        for out_ref, chunk in zip(out_refs, batch):
            out_ref[distance] = refs[distance][base : base + tile_count(chunk)]
            base += tile_count(chunk)
        if INFO_CHUNK in batch:
            out_refs[-1][distance] = refs[distance][batch_tiles(batch) - 1]


def column_kernel(batch, start_ref, weight_ref, *refs):
    sides = [refs[3 * number : 3 * number + 3] for number in range(len(batch))]
    refs = refs[3 * len(batch) :]
    out_refs, rows_refs = refs[:RING], refs[len(refs) - len(batch) :]
    place = lax.axis_index(LAT[2])
    positions = side_places(lax.axis_index(LAT[:2]))
    for chunk, side_refs, rows_ref in zip(batch, sides, rows_refs):
        count = width_of(chunk) * ROWS
        if chunk == SUMS_CHUNK:
            for side, ref in zip(positions, side_refs):
                refs[RING][side] = ref[:, count]
        for distance in range(RING):
            band = across(place, distance)
            for side, ref in zip(positions, side_refs):
                rows_ref[pl.ds((side * RING + band) * count, count)] = ref[distance, :count]

    def one_row(row, carry):
        for distance in range(RING):
            first = start_ref[distance, row]
            weights = [weight_ref[step, distance, row] for step in range(4)]
            base = 0
            for chunk, rows_ref in zip(batch, rows_refs):
                width = width_of(chunk)
                total = weights[0] * rows_ref[pl.ds(first * width, width)]
                for step in range(1, 4):
                    total = total + weights[step] * rows_ref[pl.ds((first + step) * width, width)]
                out_refs[distance][pl.ds(base + row * width, width)] = total
                base += ROWS * width
        return carry

    lax.fori_loop(0, ROWS, one_row, 0)


def field_units(field):
    found = []
    for tile in range(QUARTER):
        unit = field * QUARTER + tile
        for number, batch in enumerate(BACK):
            base = 0
            for chunk in batch:
                first, last = CHUNKS[chunk]
                if first <= unit < last:
                    found.append((number, base + unit - first, last - first))
                base += ROWS * (last - first)
    return found


def field_batches(field):
    return sorted({number for number, _, _ in field_units(field)})


def finish_kernel(field, shift_ref, weight_ref, ratio_ref, *refs):
    out_ref, turned_ref = refs[-2], refs[-1]
    batches = field_batches(field)
    place = lax.axis_index(LAT[2])
    owners = [across(place, distance) for distance in range(RING)]
    lane = lax.broadcasted_iota(jnp.int32, (8, LANES), 1)
    scale = ratio_ref[field]

    def ahead(values, step):
        moved = [pltpu.roll(value, LANES - step, 1) for value in values]
        following = moved[1:] + moved[:1]
        return [jnp.where(lane < LANES - step, here, then) for here, then in zip(moved, following)]

    def some_rows(pair, carry):
        for member in range(TOGETHER):
            row = pair * TOGETHER + member
            slot = member * 2 * TILES
            base = shift_ref[row]
            base = jnp.where(base == 0, LON - 1, base - 1)
            whole = base // LANES
            back = LANES - (base - whole * LANES)
            for distance in range(RING):
                for tile, (number, at, width) in enumerate(field_units(field)):
                    piece = refs[batches.index(number) * RING + distance][row * width + at]
                    turned_ref[slot + owners[distance] * QUARTER + tile] = piece
                    turned_ref[slot + TILES + owners[distance] * QUARTER + tile] = piece
            weights = [weight_ref[step, row] * scale for step in range(4)]
            rolled = [pltpu.roll(turned_ref[slot + whole + tile], back, 1) for tile in range(TILES)]
            lined = [jnp.where(lane < back, here, then) for here, then in zip(rolled, rolled[1:] + rolled[:1])]
            next_one = ahead(lined, 1)
            far = ahead([weights[2] * here + weights[3] * then for here, then in zip(lined, next_one)], 2)
            for tile in range(TILES):
                out_ref[row, 0, :, tile * LANES : (tile + 1) * LANES] = (
                    weights[0] * lined[tile] + weights[1] * next_one[tile] + far[tile]
                )
        return carry

    lax.fori_loop(0, ROWS // TOGETHER, some_rows, 0)


def swap(array, axis, partner):
    return lax.ppermute(array, axis, [(i, partner(i)) for i in range(lax.axis_size(axis))])


def exchange(pieces):
    received = {0: pieces[0]}
    for step in PARTNERS:
        received[step] = swap(pieces[step], LAT[2], lambda i, step=step: i ^ step)
    return [received[step] for step in range(RING)]


def both_sides(block):
    groups = lax.axis_size(LAT[:2])
    inner = swap(block, LAT[:2], lambda i: i ^ 1)
    outer = swap(block, LAT[:2], lambda i: (i + 1 if i % 2 else i - 1) % groups)
    return inner, outer


def tiles(*shape):
    return jax.ShapeDtypeStruct((*shape, 8, LANES), jnp.float32)


def per_device(fields, lat_fraction, lon_fraction, lon_shift, departure_row, extents):
    params = pltpu.CompilerParams(vmem_limit_bytes=VMEM_LIMIT)
    pieces = []
    packs = (
        (pack_first, ()),
        (pack_second, (departure_row, extents, lat_fraction, lon_fraction)),
        (pack_third, ()),
    )
    for number, (kernel, scalars) in enumerate(packs):
        pieces.append(
            pl.pallas_call(
                kernel,
                out_shape=[tiles(batch_tiles(OWN[number]))] * RING,
                in_specs=[SMEM] * len(scalars) + [VMEM],
                out_specs=[VMEM] * RING,
                compiler_params=params,
                name="pack",
            )(*scalars, fields)
        )

    own, inner, outer = {}, {}, {}
    for number, batch in enumerate(OWN):
        received = exchange(pieces[number])
        shapes = [tiles(RING, tile_count(chunk)) for chunk in batch] + [tiles(RING)] * (INFO_CHUNK in batch)
        joined = pl.pallas_call(
            partial(join_kernel, batch),
            out_shape=shapes,
            in_specs=[VMEM] * RING,
            out_specs=[VMEM] * len(shapes),
            compiler_params=params,
            name="join",
        )(*received)
        if INFO_CHUNK in batch:
            ring_info = joined[-1][:, :, :ROWS]
        for chunk, block in zip(batch, joined):
            own[chunk] = block
            inner[chunk], outer[chunk] = both_sides(block)

    ring_start = ring_info[:, 0].astype(jnp.int32)
    ring_weight = jnp.stack(cubic_weights(ring_info[:, 1]))

    gathered = []
    for batch in BACK:
        shapes = [tiles(column_tiles(batch))] * RING + [tiles(3, RING)] * (SUMS_CHUNK in batch)
        operands = [part[chunk] for chunk in batch for part in (inner, own, outer)]
        columns = pl.pallas_call(
            partial(column_kernel, batch),
            out_shape=shapes,
            in_specs=[SMEM, SMEM] + [VMEM] * len(operands),
            out_specs=[VMEM] * len(shapes),
            scratch_shapes=[
                pltpu.VMEM((3 * GROUP * width_of(chunk), 8, LANES), jnp.float32) for chunk in batch
            ],
            compiler_params=params,
            name="column",
        )(ring_start, ring_weight, *operands)
        if SUMS_CHUNK in batch:
            all_sums = columns[RING]
        gathered.append(exchange(columns[:RING]))

    total_rows = lax.axis_size(LAT) * ROWS
    group_row = lax.axis_index(LAT[:2]) * GROUP
    bands = across(lax.axis_index(LAT[2]), jnp.arange(RING, dtype=jnp.int32))
    ring_rows = bands[:, None] * ROWS + jnp.arange(ROWS, dtype=jnp.int32)[None]
    area = jnp.cos(math.pi * ((group_row + ring_rows).astype(jnp.float32) + 0.5) / total_rows - math.pi / 2.0)
    sums = all_sums[:, :, :FIELDS, :ROWS]
    lon_total = sum(cubic_weights(ring_info[:, 2]))
    before = jnp.sum(area[:, None, :] * sums[1], axis=(0, 2))
    after = jnp.zeros((FIELDS,), jnp.float32)
    for side in range(3):
        spots = side * GROUP + ring_rows
        factor = jnp.zeros((RING, ROWS), jnp.float32)
        for step in range(4):
            hit = (ring_start + step)[None, None] == spots[..., None, None]
            share = area * lon_total * ring_weight[step]
            factor = factor + jnp.sum(jnp.where(hit, share[None, None], 0.0), axis=(2, 3))
        after = after + jnp.sum(factor[:, None, :] * sums[side], axis=(0, 2))
    mass = jnp.pad(jnp.concatenate([before, after]), (0, LANES - 2 * FIELDS))
    parties = (LAT[0], LAT[1], "lev")
    spread = jnp.broadcast_to(mass[None, None], (lax.axis_size(parties), 1, LANES))
    spread = lax.all_to_all(spread, parties, 0, 0)
    mass = jnp.sum(spread, axis=(0, 1))
    ratio = mass[:FIELDS] / mass[FIELDS : 2 * FIELDS]
    lon_w = jnp.stack(cubic_weights(lon_fraction))

    result = None
    for field in range(FIELDS):
        operands = [piece for number in field_batches(field) for piece in gathered[number]]
        in_specs = [SMEM, SMEM, SMEM] + [VMEM] * len(operands)
        aliases = {}
        if result is not None:
            operands.append(result)
            in_specs.append(ANY)
            aliases = {len(in_specs) - 1: 0}
        result = pl.pallas_call(
            partial(finish_kernel, field),
            grid=(1,),
            out_shape=jax.ShapeDtypeStruct(fields.shape, jnp.float32),
            in_specs=in_specs,
            out_specs=pl.BlockSpec((ROWS, 1, 8, LON), lambda i, field=field: (0, field, 0, 0)),
            scratch_shapes=[pltpu.VMEM((TOGETHER * 2 * TILES, 8, LANES), jnp.float32)],
            input_output_aliases=aliases,
            compiler_params=params,
            name="finish",
        )(lon_shift, lon_w, ratio, *operands)
    return result


def solution(mesh):
    finer = Mesh(mesh.devices.reshape(4, 8, 4, mesh.shape["lev"]), LAT + ("lev",))
    placed = (P(LAT, None, "lev", None), P(LAT), P(LAT), P(LAT), P(LAT), P(LAT, None))
    return jax.shard_map(
        per_device,
        mesh=finer,
        in_specs=placed,
        out_specs=P(LAT, None, "lev", None),
        check_vma=False,
    )
```

```python
import math
from functools import partial

import jax
import jax.numpy as jnp
from jax import lax
from jax.experimental import pallas as pl
from jax.experimental.pallas import tpu as pltpu
from jax.sharding import Mesh
from jax.sharding import PartitionSpec as P


LAT = ("lat_0", "lat_1", "lat_2")
ROWS = 10
RING = 4
GROUP = RING * ROWS
FIELDS = 3
LANES = 128
QUARTER = 5
TILES = RING * QUARTER
LON = TILES * LANES
CHUNKS = ((0, 3), (3, 10), (10, 15))
PARTNERS = (2, 1, 3)
EARLY = 0
OWN = ((1,), (2,))
BACK = ((0,), (1,), (2,))
SUMS_CHUNK = 0
INFO_CHUNK = 2
MARKED = (SUMS_CHUNK, INFO_CHUNK)
TOGETHER = 5
VMEM_LIMIT = 12 * 1024 * 1024


VMEM = pl.BlockSpec(memory_space=pltpu.VMEM)
SMEM = pl.BlockSpec(memory_space=pltpu.SMEM)
ANY = pl.BlockSpec(memory_space=pl.ANY)


def cubic_weights(fraction):
    return (
        -fraction * (fraction - 1.0) * (fraction - 2.0) / 6.0,
        (fraction + 1.0) * (fraction - 1.0) * (fraction - 2.0) / 2.0,
        -(fraction + 1.0) * fraction * (fraction - 2.0) / 2.0,
        (fraction + 1.0) * fraction * (fraction - 1.0) / 6.0,
    )


def across(place, step):
    return jnp.bitwise_xor(place, step)


def side_places(group):
    even = 1 - lax.rem(group, 2)
    return 2 * even, 1, 2 - 2 * even


def width_of(chunk):
    first, last = CHUNKS[chunk]
    return last - first


def tile_count(chunk):
    return ROWS * width_of(chunk) + (1 if chunk in MARKED else 0)


def batch_tiles(batch):
    return sum(tile_count(chunk) for chunk in batch)


def column_tiles(batch):
    return sum(ROWS * width_of(chunk) for chunk in batch) + (1 if EARLY in batch else 0)


def copy_units(fields_ref, chunk, owner, piece_ref):
    first, last = CHUNKS[chunk]
    for unit in range(first, last):
        field, tile = divmod(unit, QUARTER)
        start = pl.multiple_of((owner * QUARTER + tile) * LANES, LANES)
        for row in range(ROWS):
            piece_ref[row * (last - first) + unit - first] = fields_ref[row, field, :, pl.ds(start, LANES)]


def copy_pieces(fields_ref, chunk, piece_refs):
    place = lax.axis_index(LAT[2])
    for distance in range(RING):
        copy_units(fields_ref, chunk, across(place, distance), piece_refs[distance])


def pack_plain(fields_ref, *piece_refs):
    copy_pieces(fields_ref, OWN[0][0], piece_refs)


def pack_early(fields_ref, early_ref):
    sub = lax.broadcasted_iota(jnp.int32, (ROWS, LANES), 0)
    lane = lax.broadcasted_iota(jnp.int32, (ROWS, LANES), 1)
    sums_sub = lax.broadcasted_iota(jnp.int32, (8, LANES), 0)
    sums = jnp.zeros((8, LANES), jnp.float32)
    for field in range(FIELDS):
        total = fields_ref[:, field, :, 0:LANES]
        for tile in range(1, TILES):
            total = total + fields_ref[:, field, :, tile * LANES : (tile + 1) * LANES]
        by_row = jnp.sum(jnp.sum(total, axis=1), axis=1, keepdims=True)
        in_lanes = jnp.sum(jnp.where(sub == lane, by_row, 0.0), axis=0, keepdims=True)
        sums = jnp.where(sums_sub == field, in_lanes, sums)
    copy_pieces(fields_ref, EARLY, [early_ref.at[distance] for distance in range(RING)])
    for distance in range(RING):
        early_ref[distance, tile_count(EARLY) - 1] = sums


def pack_marked(departure_ref, extents_ref, lat_ref, lon_ref, fields_ref, *piece_refs):
    first_row = lax.axis_index(LAT) * ROWS
    group_row = lax.axis_index(LAT[:2]) * GROUP
    low_bound = first_row - extents_ref[0, 0] * ROWS + 1
    high_bound = first_row + ROWS - 3 + extents_ref[0, 1] * ROWS
    info_sub = lax.broadcasted_iota(jnp.int32, (8, LANES), 0)
    info_lane = lax.broadcasted_iota(jnp.int32, (8, LANES), 1)
    starts = jnp.zeros((8, LANES), jnp.int32)
    info = jnp.zeros((8, LANES), jnp.float32)
    for row in range(ROWS):
        departure = jnp.clip(departure_ref[row], low_bound, high_bound)
        departure = jnp.clip(departure, 1, RING * 32 * ROWS - 3)
        here = info_lane == row
        starts = jnp.where(here, departure - 1 - (group_row - GROUP), starts)
        info = jnp.where(here & (info_sub == 1), lat_ref[row], info)
        info = jnp.where(here & (info_sub == 2), lon_ref[row], info)
    info = jnp.where(info_sub == 0, starts.astype(jnp.float32), info)
    copy_pieces(fields_ref, INFO_CHUNK, piece_refs)
    for ref in piece_refs:
        ref[tile_count(INFO_CHUNK) - 1] = info


def bundle_kernel(*refs):
    count = ROWS * width_of(EARLY)
    positions = side_places(lax.axis_index(LAT[:2]))
    for side in range(3):
        refs[-1][positions[side]] = refs[side][0, count]
        for distance in range(RING):
            refs[3 + distance][side * count : (side + 1) * count] = refs[side][distance, :count]


def join_kernel(batch, *refs):
    out_refs = refs[RING:]
    for distance in range(RING):
        base = 0
        for out_ref, chunk in zip(out_refs, batch):
            out_ref[distance] = refs[distance][base : base + tile_count(chunk)]
            base += tile_count(chunk)
        if INFO_CHUNK in batch:
            out_refs[-1][distance] = refs[distance][batch_tiles(batch) - 1]


def column_kernel(batch, start_ref, weight_ref, *refs):
    sides = []
    for chunk in batch:
        taken = RING if chunk == EARLY else 3
        sides.append(refs[:taken])
        refs = refs[taken:]
    if EARLY in batch:
        for out_ref in refs[1 : RING + 1]:
            out_ref[column_tiles(batch) - 1] = refs[0][...]
        refs = refs[1:]
    out_refs, rows_refs = refs[:RING], refs[RING:]
    place = lax.axis_index(LAT[2])
    positions = side_places(lax.axis_index(LAT[:2]))
    for chunk, side_refs, rows_ref in zip(batch, sides, rows_refs):
        count = width_of(chunk) * ROWS
        for distance in range(RING):
            band = across(place, distance)
            for side in range(3):
                if chunk == EARLY:
                    block = side_refs[distance][side * count : (side + 1) * count]
                else:
                    block = side_refs[side][distance, :count]
                rows_ref[pl.ds((positions[side] * RING + band) * count, count)] = block

    def one_row(row, carry):
        for distance in range(RING):
            first = start_ref[distance, row]
            weights = [weight_ref[step, distance, row] for step in range(4)]
            base = 0
            for chunk, rows_ref in zip(batch, rows_refs):
                width = width_of(chunk)
                total = weights[0] * rows_ref[pl.ds(first * width, width)]
                for step in range(1, 4):
                    total = total + weights[step] * rows_ref[pl.ds((first + step) * width, width)]
                out_refs[distance][pl.ds(base + row * width, width)] = total
                base += ROWS * width
        return carry

    lax.fori_loop(0, ROWS, one_row, 0)


def field_units(field):
    found = []
    for tile in range(QUARTER):
        unit = field * QUARTER + tile
        for number, batch in enumerate(BACK):
            base = 0
            for chunk in batch:
                first, last = CHUNKS[chunk]
                if first <= unit < last:
                    found.append((number, base + unit - first, last - first))
                base += ROWS * (last - first)
    return found


def field_batches(field):
    return sorted({number for number, _, _ in field_units(field)})


def finish_kernel(field, shift_ref, weight_ref, ratio_ref, *refs):
    out_ref, turned_ref = refs[-2], refs[-1]
    batches = field_batches(field)
    place = lax.axis_index(LAT[2])
    owners = [across(place, distance) for distance in range(RING)]
    lane = lax.broadcasted_iota(jnp.int32, (8, LANES), 1)
    scale = ratio_ref[field]

    def ahead(values, step):
        moved = [pltpu.roll(value, LANES - step, 1) for value in values]
        following = moved[1:] + moved[:1]
        return [jnp.where(lane < LANES - step, here, then) for here, then in zip(moved, following)]

    def some_rows(pair, carry):
        for member in range(TOGETHER):
            row = pair * TOGETHER + member
            slot = member * 2 * TILES
            base = shift_ref[row]
            base = jnp.where(base == 0, LON - 1, base - 1)
            whole = base // LANES
            back = LANES - (base - whole * LANES)
            for distance in range(RING):
                for tile, (number, at, width) in enumerate(field_units(field)):
                    piece = refs[batches.index(number) * RING + distance][row * width + at]
                    turned_ref[slot + owners[distance] * QUARTER + tile] = piece
                    turned_ref[slot + TILES + owners[distance] * QUARTER + tile] = piece
            weights = [weight_ref[step, row] * scale for step in range(4)]
            rolled = [pltpu.roll(turned_ref[slot + whole + tile], back, 1) for tile in range(TILES)]
            lined = [jnp.where(lane < back, here, then) for here, then in zip(rolled, rolled[1:] + rolled[:1])]
            next_one = ahead(lined, 1)
            far = ahead([weights[2] * here + weights[3] * then for here, then in zip(lined, next_one)], 2)
            for tile in range(TILES):
                out_ref[row, 0, :, tile * LANES : (tile + 1) * LANES] = (
                    weights[0] * lined[tile] + weights[1] * next_one[tile] + far[tile]
                )
        return carry

    lax.fori_loop(0, ROWS // TOGETHER, some_rows, 0)


def swap(array, axis, partner):
    return lax.ppermute(array, axis, [(i, partner(i)) for i in range(lax.axis_size(axis))])


def exchange(pieces):
    received = {0: pieces[0]}
    for step in PARTNERS:
        received[step] = swap(pieces[step], LAT[2], lambda i, step=step: i ^ step)
    return [received[step] for step in range(RING)]


def both_sides(block):
    groups = lax.axis_size(LAT[:2])
    inner = swap(block, LAT[:2], lambda i: i ^ 1)
    outer = swap(block, LAT[:2], lambda i: (i + 1 if i % 2 else i - 1) % groups)
    return inner, outer


def tiles(*shape):
    return jax.ShapeDtypeStruct((*shape, 8, LANES), jnp.float32)


def per_device(fields, lat_fraction, lon_fraction, lon_shift, departure_row, extents):
    params = pltpu.CompilerParams(vmem_limit_bytes=VMEM_LIMIT)

    def pack(kernel, shapes, *operands):
        return pl.pallas_call(
            kernel,
            out_shape=shapes,
            in_specs=[SMEM] * (len(operands) - 1) + [VMEM],
            out_specs=[VMEM] * len(shapes),
            compiler_params=params,
            name="pack",
        )(*operands)

    pieces = [pack(pack_plain, [tiles(batch_tiles(OWN[0]))] * RING, fields)]
    early = pack(pack_early, [tiles(RING, tile_count(EARLY))], fields)[0]
    scalars = (departure_row, extents, lat_fraction, lon_fraction)
    pieces.append(pack(pack_marked, [tiles(batch_tiles(OWN[1]))] * RING, *scalars, fields))

    early_inner, early_outer = both_sides(early)
    bundles = pl.pallas_call(
        bundle_kernel,
        out_shape=[tiles(3 * ROWS * width_of(EARLY))] * RING + [tiles(3)],
        in_specs=[VMEM] * 3,
        out_specs=[VMEM] * (RING + 1),
        compiler_params=params,
        name="bundle",
    )(early_inner, early, early_outer)
    sums = bundles[RING][:, :FIELDS, :ROWS]
    bundles = exchange(bundles[:RING])

    own, inner, outer = {}, {}, {}
    for number, batch in enumerate(OWN):
        received = exchange(pieces[number])
        shapes = [tiles(RING, tile_count(chunk)) for chunk in batch] + [tiles(RING)] * (INFO_CHUNK in batch)
        joined = pl.pallas_call(
            partial(join_kernel, batch),
            out_shape=shapes,
            in_specs=[VMEM] * RING,
            out_specs=[VMEM] * len(shapes),
            compiler_params=params,
            name="join",
        )(*received)
        if INFO_CHUNK in batch:
            ring_info = joined[-1][:, :, :ROWS]
        for chunk, block in zip(batch, joined):
            own[chunk] = block
            inner[chunk], outer[chunk] = both_sides(block)

    ring_start = ring_info[:, 0].astype(jnp.int32)
    ring_weight = jnp.stack(cubic_weights(ring_info[:, 1]))

    total_rows = lax.axis_size(LAT) * ROWS
    group_row = lax.axis_index(LAT[:2]) * GROUP
    place = lax.axis_index(LAT[2])
    bands = across(place, jnp.arange(RING, dtype=jnp.int32))
    ring_rows = bands[:, None] * ROWS + jnp.arange(ROWS, dtype=jnp.int32)[None]
    area = jnp.cos(math.pi * ((group_row + ring_rows).astype(jnp.float32) + 0.5) / total_rows - math.pi / 2.0)
    lon_total = sum(cubic_weights(ring_info[:, 2]))
    spots = jnp.arange(3, dtype=jnp.int32)[:, None] * GROUP + ring_rows[0][None]
    factor = jnp.zeros((3, ROWS), jnp.float32)
    for step in range(4):
        hit = (ring_start + step)[None, None] == spots[..., None, None]
        share = area * lon_total * ring_weight[step]
        factor = factor + jnp.sum(jnp.where(hit, share[None, None], 0.0), axis=(2, 3))
    before = jnp.sum(area[0][None] * sums[1], axis=1)
    after = jnp.sum(factor[:, None, :] * sums, axis=(0, 2))
    mass = jnp.pad(jnp.concatenate([before, after]), (0, LANES - 2 * FIELDS))
    parties = (LAT[0], LAT[1], "lev")
    spread = jnp.broadcast_to(mass[None, None], (lax.axis_size(parties), 1, LANES))
    spread = lax.all_to_all(spread, parties, 0, 0)
    column_mass = jnp.broadcast_to(jnp.sum(spread, axis=0), (8, LANES))

    gathered = []
    for batch in BACK:
        shapes = [tiles(column_tiles(batch))] * RING
        operands = []
        for chunk in batch:
            operands += bundles if chunk == EARLY else [inner[chunk], own[chunk], outer[chunk]]
        if EARLY in batch:
            operands.append(column_mass)
        columns = pl.pallas_call(
            partial(column_kernel, batch),
            out_shape=shapes,
            in_specs=[SMEM, SMEM] + [VMEM] * len(operands),
            out_specs=[VMEM] * len(shapes),
            scratch_shapes=[
                pltpu.VMEM((3 * GROUP * width_of(chunk), 8, LANES), jnp.float32) for chunk in batch
            ],
            compiler_params=params,
            name="column",
        )(ring_start, ring_weight, *operands)
        gathered.append(exchange(columns))

    mass = sum(piece[-1, 0, : 2 * FIELDS] for piece in gathered[0])
    ratio = mass[:FIELDS] / mass[FIELDS:]
    lon_w = jnp.stack(cubic_weights(lon_fraction))

    result = None
    for field in range(FIELDS):
        operands = [piece for number in field_batches(field) for piece in gathered[number]]
        in_specs = [SMEM, SMEM, SMEM] + [VMEM] * len(operands)
        aliases = {}
        if result is not None:
            operands.append(result)
            in_specs.append(ANY)
            aliases = {len(in_specs) - 1: 0}
        result = pl.pallas_call(
            partial(finish_kernel, field),
            grid=(1,),
            out_shape=jax.ShapeDtypeStruct(fields.shape, jnp.float32),
            in_specs=in_specs,
            out_specs=pl.BlockSpec((ROWS, 1, 8, LON), lambda i, field=field: (0, field, 0, 0)),
            scratch_shapes=[pltpu.VMEM((TOGETHER * 2 * TILES, 8, LANES), jnp.float32)],
            input_output_aliases=aliases,
            compiler_params=params,
            name="finish",
        )(lon_shift, lon_w, ratio, *operands)
    return result


def solution(mesh):
    finer = Mesh(mesh.devices.reshape(4, 8, 4, mesh.shape["lev"]), LAT + ("lev",))
    placed = (P(LAT, None, "lev", None), P(LAT), P(LAT), P(LAT), P(LAT), P(LAT, None))
    return jax.shard_map(
        per_device,
        mesh=finer,
        in_specs=placed,
        out_specs=P(LAT, None, "lev", None),
        check_vma=False,
    )
```

```python
import math
from functools import partial

import jax
import jax.numpy as jnp
from jax import lax
from jax.experimental import pallas as pl
from jax.experimental.pallas import tpu as pltpu
from jax.sharding import Mesh
from jax.sharding import PartitionSpec as P


LAT = ("lat_0", "lat_1", "lat_2")
ROWS = 10
RING = 4
GROUP = RING * ROWS
FIELDS = 3
LANES = 128
QUARTER = 5
TILES = RING * QUARTER
LON = TILES * LANES
CHUNKS = ((0, 3), (3, 10), (10, 15))
PARTNERS = (1, 3, 2)
EARLY = 0
OWN = ((1,), (2,))
BACK = ((0, 1), (2,))
SUMS_CHUNK = 0
INFO_CHUNK = 2
MARKED = (SUMS_CHUNK, INFO_CHUNK)
TOGETHER = 5
VMEM_LIMIT = 12 * 1024 * 1024


VMEM = pl.BlockSpec(memory_space=pltpu.VMEM)
SMEM = pl.BlockSpec(memory_space=pltpu.SMEM)
ANY = pl.BlockSpec(memory_space=pl.ANY)


def cubic_weights(fraction):
    return (
        -fraction * (fraction - 1.0) * (fraction - 2.0) / 6.0,
        (fraction + 1.0) * (fraction - 1.0) * (fraction - 2.0) / 2.0,
        -(fraction + 1.0) * fraction * (fraction - 2.0) / 2.0,
        (fraction + 1.0) * fraction * (fraction - 1.0) / 6.0,
    )


def across(place, step):
    return jnp.bitwise_xor(place, step)


def side_places(group):
    even = 1 - lax.rem(group, 2)
    return 2 * even, 1, 2 - 2 * even


def width_of(chunk):
    first, last = CHUNKS[chunk]
    return last - first


def tile_count(chunk):
    return ROWS * width_of(chunk) + (1 if chunk in MARKED else 0)


def batch_tiles(batch):
    return sum(tile_count(chunk) for chunk in batch)


def column_tiles(batch):
    return sum(ROWS * width_of(chunk) for chunk in batch)


def copy_units(fields_ref, chunk, owner, piece_ref):
    first, last = CHUNKS[chunk]
    for unit in range(first, last):
        field, tile = divmod(unit, QUARTER)
        start = pl.multiple_of((owner * QUARTER + tile) * LANES, LANES)
        for row in range(ROWS):
            piece_ref[row * (last - first) + unit - first] = fields_ref[row, field, :, pl.ds(start, LANES)]


def copy_pieces(fields_ref, chunk, piece_refs):
    place = lax.axis_index(LAT[2])
    for distance in range(RING):
        copy_units(fields_ref, chunk, across(place, distance), piece_refs[distance])


def pack_plain(fields_ref, *piece_refs):
    copy_pieces(fields_ref, OWN[0][0], piece_refs)


def pack_early(fields_ref, early_ref):
    sub = lax.broadcasted_iota(jnp.int32, (ROWS, LANES), 0)
    lane = lax.broadcasted_iota(jnp.int32, (ROWS, LANES), 1)
    sums_sub = lax.broadcasted_iota(jnp.int32, (8, LANES), 0)
    sums = jnp.zeros((8, LANES), jnp.float32)
    for field in range(FIELDS):
        total = fields_ref[:, field, :, 0:LANES]
        for tile in range(1, TILES):
            total = total + fields_ref[:, field, :, tile * LANES : (tile + 1) * LANES]
        by_row = jnp.sum(jnp.sum(total, axis=1), axis=1, keepdims=True)
        in_lanes = jnp.sum(jnp.where(sub == lane, by_row, 0.0), axis=0, keepdims=True)
        sums = jnp.where(sums_sub == field, in_lanes, sums)
    copy_pieces(fields_ref, EARLY, [early_ref.at[distance] for distance in range(RING)])
    for distance in range(RING):
        early_ref[distance, tile_count(EARLY) - 1] = sums


def pack_marked(departure_ref, extents_ref, lat_ref, lon_ref, fields_ref, *piece_refs):
    first_row = lax.axis_index(LAT) * ROWS
    group_row = lax.axis_index(LAT[:2]) * GROUP
    low_bound = first_row - extents_ref[0, 0] * ROWS + 1
    high_bound = first_row + ROWS - 3 + extents_ref[0, 1] * ROWS
    info_sub = lax.broadcasted_iota(jnp.int32, (8, LANES), 0)
    info_lane = lax.broadcasted_iota(jnp.int32, (8, LANES), 1)
    starts = jnp.zeros((8, LANES), jnp.int32)
    info = jnp.zeros((8, LANES), jnp.float32)
    for row in range(ROWS):
        departure = jnp.clip(departure_ref[row], low_bound, high_bound)
        departure = jnp.clip(departure, 1, RING * 32 * ROWS - 3)
        here = info_lane == row
        starts = jnp.where(here, departure - 1 - (group_row - GROUP), starts)
        info = jnp.where(here & (info_sub == 1), lat_ref[row], info)
        info = jnp.where(here & (info_sub == 2), lon_ref[row], info)
    info = jnp.where(info_sub == 0, starts.astype(jnp.float32), info)
    copy_pieces(fields_ref, INFO_CHUNK, piece_refs)
    for ref in piece_refs:
        ref[tile_count(INFO_CHUNK) - 1] = info


def bundle_kernel(*refs):
    count = tile_count(EARLY)
    for distance in range(RING):
        for side in range(3):
            refs[3 + distance][side * count : (side + 1) * count] = refs[side][distance]


def join_kernel(batch, *refs):
    out_refs = refs[RING:]
    for distance in range(RING):
        base = 0
        for out_ref, chunk in zip(out_refs, batch):
            out_ref[distance] = refs[distance][base : base + tile_count(chunk)]
            base += tile_count(chunk)
        if INFO_CHUNK in batch:
            out_refs[-1][distance] = refs[distance][batch_tiles(batch) - 1]


def column_kernel(batch, start_ref, weight_ref, *refs):
    sides = []
    for chunk in batch:
        taken = RING if chunk == EARLY else 3
        sides.append(refs[:taken])
        refs = refs[taken:]
    out_refs, rows_refs = refs[:RING], refs[len(refs) - len(batch) :]
    place = lax.axis_index(LAT[2])
    positions = side_places(lax.axis_index(LAT[:2]))
    for chunk, side_refs, rows_ref in zip(batch, sides, rows_refs):
        count = width_of(chunk) * ROWS
        span = tile_count(chunk)
        for distance in range(RING):
            band = across(place, distance)
            for side in range(3):
                if chunk == EARLY:
                    ref, base = side_refs[distance], side * span
                    block = ref[base : base + count]
                    refs[RING][positions[side], distance] = ref[base + count]
                else:
                    block = side_refs[side][distance, :count]
                rows_ref[pl.ds((positions[side] * RING + band) * count, count)] = block

    def one_row(row, carry):
        for distance in range(RING):
            first = start_ref[distance, row]
            weights = [weight_ref[step, distance, row] for step in range(4)]
            base = 0
            for chunk, rows_ref in zip(batch, rows_refs):
                width = width_of(chunk)
                total = weights[0] * rows_ref[pl.ds(first * width, width)]
                for step in range(1, 4):
                    total = total + weights[step] * rows_ref[pl.ds((first + step) * width, width)]
                out_refs[distance][pl.ds(base + row * width, width)] = total
                base += ROWS * width
        return carry

    lax.fori_loop(0, ROWS, one_row, 0)


def field_units(field):
    found = []
    for tile in range(QUARTER):
        unit = field * QUARTER + tile
        for number, batch in enumerate(BACK):
            base = 0
            for chunk in batch:
                first, last = CHUNKS[chunk]
                if first <= unit < last:
                    found.append((number, base + unit - first, last - first))
                base += ROWS * (last - first)
    return found


def field_batches(field):
    return sorted({number for number, _, _ in field_units(field)})


def finish_kernel(field, shift_ref, weight_ref, ratio_ref, *refs):
    out_ref, turned_ref = refs[-2], refs[-1]
    batches = field_batches(field)
    place = lax.axis_index(LAT[2])
    owners = [across(place, distance) for distance in range(RING)]
    lane = lax.broadcasted_iota(jnp.int32, (8, LANES), 1)
    scale = ratio_ref[field]

    def ahead(values, step):
        moved = [pltpu.roll(value, LANES - step, 1) for value in values]
        following = moved[1:] + moved[:1]
        return [jnp.where(lane < LANES - step, here, then) for here, then in zip(moved, following)]

    def some_rows(pair, carry):
        for member in range(TOGETHER):
            row = pair * TOGETHER + member
            slot = member * 2 * TILES
            base = shift_ref[row]
            base = jnp.where(base == 0, LON - 1, base - 1)
            whole = base // LANES
            back = LANES - (base - whole * LANES)
            for distance in range(RING):
                for tile, (number, at, width) in enumerate(field_units(field)):
                    piece = refs[batches.index(number) * RING + distance][row * width + at]
                    turned_ref[slot + owners[distance] * QUARTER + tile] = piece
                    turned_ref[slot + TILES + owners[distance] * QUARTER + tile] = piece
            weights = [weight_ref[step, row] * scale for step in range(4)]
            rolled = [pltpu.roll(turned_ref[slot + whole + tile], back, 1) for tile in range(TILES)]
            lined = [jnp.where(lane < back, here, then) for here, then in zip(rolled, rolled[1:] + rolled[:1])]
            next_one = ahead(lined, 1)
            far = ahead([weights[2] * here + weights[3] * then for here, then in zip(lined, next_one)], 2)
            for tile in range(TILES):
                out_ref[row, 0, :, tile * LANES : (tile + 1) * LANES] = (
                    weights[0] * lined[tile] + weights[1] * next_one[tile] + far[tile]
                )
        return carry

    lax.fori_loop(0, ROWS // TOGETHER, some_rows, 0)


def swap(array, axis, partner):
    return lax.ppermute(array, axis, [(i, partner(i)) for i in range(lax.axis_size(axis))])


def exchange(pieces):
    received = {0: pieces[0]}
    for step in PARTNERS:
        received[step] = swap(pieces[step], LAT[2], lambda i, step=step: i ^ step)
    return [received[step] for step in range(RING)]


def both_sides(block):
    groups = lax.axis_size(LAT[:2])
    inner = swap(block, LAT[:2], lambda i: i ^ 1)
    outer = swap(block, LAT[:2], lambda i: (i + 1 if i % 2 else i - 1) % groups)
    return inner, outer


def tiles(*shape):
    return jax.ShapeDtypeStruct((*shape, 8, LANES), jnp.float32)


def per_device(fields, lat_fraction, lon_fraction, lon_shift, departure_row, extents):
    params = pltpu.CompilerParams(vmem_limit_bytes=VMEM_LIMIT)

    def pack(kernel, shapes, *operands):
        return pl.pallas_call(
            kernel,
            out_shape=shapes,
            in_specs=[SMEM] * (len(operands) - 1) + [VMEM],
            out_specs=[VMEM] * len(shapes),
            compiler_params=params,
            name="pack",
        )(*operands)

    pieces = [pack(pack_plain, [tiles(batch_tiles(OWN[0]))] * RING, fields)]
    early = pack(pack_early, [tiles(RING, tile_count(EARLY))], fields)[0]
    scalars = (departure_row, extents, lat_fraction, lon_fraction)
    pieces.append(pack(pack_marked, [tiles(batch_tiles(OWN[1]))] * RING, *scalars, fields))

    early_inner, early_outer = both_sides(early)
    bundles = pl.pallas_call(
        bundle_kernel,
        out_shape=[tiles(3 * tile_count(EARLY))] * RING,
        in_specs=[VMEM] * 3,
        out_specs=[VMEM] * RING,
        compiler_params=params,
        name="bundle",
    )(early_inner, early, early_outer)
    bundles = exchange(bundles)

    own, inner, outer = {}, {}, {}
    for number, batch in enumerate(OWN):
        received = exchange(pieces[number])
        shapes = [tiles(RING, tile_count(chunk)) for chunk in batch] + [tiles(RING)] * (INFO_CHUNK in batch)
        joined = pl.pallas_call(
            partial(join_kernel, batch),
            out_shape=shapes,
            in_specs=[VMEM] * RING,
            out_specs=[VMEM] * len(shapes),
            compiler_params=params,
            name="join",
        )(*received)
        if INFO_CHUNK in batch:
            ring_info = joined[-1][:, :, :ROWS]
        for chunk, block in zip(batch, joined):
            own[chunk] = block
            inner[chunk], outer[chunk] = both_sides(block)

    ring_start = ring_info[:, 0].astype(jnp.int32)
    ring_weight = jnp.stack(cubic_weights(ring_info[:, 1]))

    gathered = []
    for batch in BACK:
        shapes = [tiles(column_tiles(batch))] * RING + [tiles(3, RING)] * (SUMS_CHUNK in batch)
        operands = []
        for chunk in batch:
            operands += bundles if chunk == EARLY else [inner[chunk], own[chunk], outer[chunk]]
        columns = pl.pallas_call(
            partial(column_kernel, batch),
            out_shape=shapes,
            in_specs=[SMEM, SMEM] + [VMEM] * len(operands),
            out_specs=[VMEM] * len(shapes),
            scratch_shapes=[
                pltpu.VMEM((3 * GROUP * width_of(chunk), 8, LANES), jnp.float32) for chunk in batch
            ],
            compiler_params=params,
            name="column",
        )(ring_start, ring_weight, *operands)
        if SUMS_CHUNK in batch:
            all_sums = columns[RING]
        gathered.append(exchange(columns[:RING]))

    total_rows = lax.axis_size(LAT) * ROWS
    group_row = lax.axis_index(LAT[:2]) * GROUP
    bands = across(lax.axis_index(LAT[2]), jnp.arange(RING, dtype=jnp.int32))
    ring_rows = bands[:, None] * ROWS + jnp.arange(ROWS, dtype=jnp.int32)[None]
    area = jnp.cos(math.pi * ((group_row + ring_rows).astype(jnp.float32) + 0.5) / total_rows - math.pi / 2.0)
    sums = all_sums[:, :, :FIELDS, :ROWS]
    lon_total = sum(cubic_weights(ring_info[:, 2]))
    before = jnp.sum(area[:, None, :] * sums[1], axis=(0, 2))
    after = jnp.zeros((FIELDS,), jnp.float32)
    for side in range(3):
        spots = side * GROUP + ring_rows
        factor = jnp.zeros((RING, ROWS), jnp.float32)
        for step in range(4):
            hit = (ring_start + step)[None, None] == spots[..., None, None]
            share = area * lon_total * ring_weight[step]
            factor = factor + jnp.sum(jnp.where(hit, share[None, None], 0.0), axis=(2, 3))
        after = after + jnp.sum(factor[:, None, :] * sums[side], axis=(0, 2))
    mass = jnp.pad(jnp.concatenate([before, after]), (0, LANES - 2 * FIELDS))
    parties = (LAT[0], LAT[1], "lev")
    spread = jnp.broadcast_to(mass[None, None], (lax.axis_size(parties), 1, LANES))
    spread = lax.all_to_all(spread, parties, 0, 0)
    mass = jnp.sum(spread, axis=(0, 1))
    ratio = mass[:FIELDS] / mass[FIELDS : 2 * FIELDS]
    lon_w = jnp.stack(cubic_weights(lon_fraction))

    result = None
    for field in range(FIELDS):
        operands = [piece for number in field_batches(field) for piece in gathered[number]]
        in_specs = [SMEM, SMEM, SMEM] + [VMEM] * len(operands)
        aliases = {}
        if result is not None:
            operands.append(result)
            in_specs.append(ANY)
            aliases = {len(in_specs) - 1: 0}
        result = pl.pallas_call(
            partial(finish_kernel, field),
            grid=(1,),
            out_shape=jax.ShapeDtypeStruct(fields.shape, jnp.float32),
            in_specs=in_specs,
            out_specs=pl.BlockSpec((ROWS, 1, 8, LON), lambda i, field=field: (0, field, 0, 0)),
            scratch_shapes=[pltpu.VMEM((TOGETHER * 2 * TILES, 8, LANES), jnp.float32)],
            input_output_aliases=aliases,
            compiler_params=params,
            name="finish",
        )(lon_shift, lon_w, ratio, *operands)
    return result


def solution(mesh):
    finer = Mesh(mesh.devices.reshape(4, 8, 4, mesh.shape["lev"]), LAT + ("lev",))
    placed = (P(LAT, None, "lev", None), P(LAT), P(LAT), P(LAT), P(LAT), P(LAT, None))
    return jax.shard_map(
        per_device,
        mesh=finer,
        in_specs=placed,
        out_specs=P(LAT, None, "lev", None),
        check_vma=False,
    )
```
